128 devices in a mesh: lat: 8 (over y, core), lon: 16 (over z, x).
Axes of the slice: x: 4, y: 4, z: 4, core: 2. Of those that a mesh axis runs over, the one named last changes fastest.
Arguments:
- coarse: bfloat16 [122880, 1104], P(('lat', 'lon')), may hold values from -6 to 6
- w_mix: bfloat16 [69, 64], replicated, may hold values from -0.75 to 0.75
- interp: bfloat16 [16, 256], replicated, may hold values from -1.5 to 1.5
- kernel: bfloat16 [3, 3, 64, 64], replicated, may hold values from -0.25 to 0.25
- bias: float32 [64], replicated, may hold values from -3 to 3
- block_ids: int32 [128, 144], replicated, may hold values from 0 to 122879, as said below
- valid: int32 [128, 144], replicated, may hold values from 0 to 1, as said below
Outputs:
- fine_out: bfloat16 [64, 2304, 2048], P(None, 'lat', 'lon')
The draws below stay inside these ranges and needn't reach their ends.
Inputs may be any that keep to these rules, and one draw needn't show every extreme that they name: `block_ids`: the coarse grid has 192 block rows and 640 block columns, held block-cyclically: block (r, c) is row ((r mod 8) * 16 + c mod 16) * 960 + (r div 8) * 40 + c div 16 of coarse. Slot p of tile t holds block (r0 + (t div 16) * 18 + p div 8, (c0 + (t mod 16) * 8 + p mod 8) mod (640)), with offsets r0 and c0 common to all tiles. Among the valid slots of one tile at most 3 name blocks of one device, and in every tile exactly 3 valid slots name blocks of some one device. Every tile has 3 or more valid slots.
All inputs are finite; a program needn't handle non-finite values.
Results may differ from the reference program's by a relative error of at most 0.0055.
Values may be sent and summed in bfloat16 or wider, within the bound.
A program may use at most 192 MiB of HBM per device.

```python
import jax
import jax.numpy as jnp
from jax import lax

C_IN = 69
C = 64
CB_ROWS = 24
CB_COLS = 40
PR = 18
PC = 8
CB_DEV = 960
PATCHES = 144
TH = 288
TW = 128
TILES = 128
BLOCKS = 122880
N_LAT = 8
N_LON = 16
DEVICES = 128


def route_table(key):
    base = jax.random.fold_in(key, 11)
    keys = jax.random.split(base, 6)
    grid_cols = N_LON * CB_COLS
    row_start = jax.random.randint(keys[0], (), 0, N_LAT * (CB_ROWS - PR) + 1)
    col_start = jax.random.randint(keys[1], (), 0, grid_cols)
    tiles = jnp.arange(DEVICES, dtype=jnp.int32)
    tile_lat = tiles // N_LON
    tile_lon = tiles % N_LON
    slots = jnp.arange(PATCHES, dtype=jnp.int32)
    patch_row = slots // PC
    patch_col = slots % PC
    rows = row_start + tile_lat[:, None] * PR + patch_row[None, :]
    cols = (col_start + tile_lon[:, None] * PC + patch_col[None, :]) % grid_cols
    owner = rows % N_LAT * N_LON + cols % N_LON
    local = rows // N_LAT * CB_COLS + cols // N_LON
    ids = (owner * CB_DEV + local).astype(jnp.int32)
    slope_row = jax.random.randint(keys[2], (DEVICES, 1), -3, 4)
    slope_col = jax.random.randint(keys[3], (DEVICES, 1), -3, 4)
    rough = jax.random.randint(keys[4], (DEVICES, PATCHES), 0, 4)
    cut = jax.random.randint(keys[5], (DEVICES, 1), -2 * PC, PC // 2 + 1)
    score = slope_row * (patch_row[None, :] - PR // 2) + slope_col * (patch_col[None, :] - PC // 2) + rough
    forced = owner == owner[:, :1]
    live = ((score >= cut) | forced).astype(jnp.int32)
    return (ids, live)


def draw_block_ids(key, part):
    return route_table(key)[0]


def draw_valid(key, part):
    return route_table(key)[1]


def shard_levels(own_key, shape, shards, least, largest):
    def one(position, shards_of):
        heights = jax.random.uniform(jax.random.fold_in(jax.random.fold_in(own_key, 6), position), (shards_of,), jnp.float32, least / len(shards), largest / len(shards))
        return jnp.repeat(jnp.exp(heights), shape[position] // shards_of).reshape((-1,) + (1,) * (len(shape) - position - 1))

    loudness = one(*shards[0])
    for cut in shards[1:]:
        loudness = loudness * one(*cut)
    return loudness


def gaussian(stream_key, extent, scale, bound, cuts=(), kind=jnp.bfloat16):
    entries = jax.random.normal(stream_key, extent, jnp.float32) * scale
    if len(cuts) > 0:
        entries = shard_levels(stream_key, extent, cuts, -0.22, 0.18) * entries
    return jnp.clip(entries, min=-bound, max=bound).astype(kind)


def setup_inputs(seed: int = 0) -> dict:
    arg_keys = jax.random.split(jax.random.key(seed), 8)
    return {
        "coarse": gaussian(arg_keys[0], (BLOCKS, 16 * C_IN), 1.0, 6.0, ((0, 128),)),
        "w_mix": gaussian(arg_keys[1], (C_IN, C), C_IN ** -0.5, 0.75),
        "interp": gaussian(arg_keys[2], (16, 256), 16 ** -0.5, 1.5),
        "kernel": gaussian(arg_keys[3], (3, 3, C, C), (9 * C) ** -0.5, 0.25),
        "bias": gaussian(arg_keys[4], (C,), 0.5, 3.0, (), jnp.float32),
        "block_ids": draw_block_ids(jax.random.fold_in(arg_keys[7], 71), 0),
        "valid": draw_valid(jax.random.fold_in(arg_keys[7], 71), 0),
    }


def mix_rows(rows, w_mix):
    count = rows.shape[0]
    flat = rows.reshape(count * 16, C_IN)
    mapped = jnp.dot(flat, w_mix, preferred_element_type=jnp.float32).astype(jnp.bfloat16)
    return mapped.reshape(count, 16, C)


def reference(coarse, w_mix, interp, kernel, bias, block_ids, valid):
    mixed = mix_rows(coarse, w_mix)
    interp_f = interp.astype(jnp.float32)

    def tile_image(tile):
        picked = mixed[block_ids[tile]].astype(jnp.float32)
        fine = jnp.einsum('pkc,kf->pcf', picked, interp_f).astype(jnp.bfloat16)
        fine = fine * valid[tile][:, None, None].astype(jnp.bfloat16)
        fine = fine.reshape(PR, PC, C, 16, 16).transpose(2, 0, 3, 1, 4)
        return fine.reshape(C, TH, TW)

    tiles = lax.map(tile_image, jnp.arange(TILES, dtype=jnp.int32))
    field = tiles.reshape(N_LAT, N_LON, C, TH, TW).transpose(2, 0, 3, 1, 4).reshape(C, N_LAT * TH, N_LON * TW)
    land = valid.astype(jnp.float32).reshape(N_LAT, N_LON, PR, PC)
    land = jnp.repeat(jnp.repeat(land, 16, axis=2), 16, axis=3)
    land = land.transpose(0, 2, 1, 3).reshape(N_LAT * TH, N_LON * TW)
    padded = jnp.pad(field, ((0, 0), (1, 1), (1, 1)))
    kernel_f = kernel.astype(jnp.float32)
    width = N_LON * TW

    def band(index):
        rows = lax.dynamic_slice_in_dim(padded, (index * TH).astype(jnp.int32), TH + 2, 1).astype(jnp.float32)
        total = jnp.zeros((C, TH, width), jnp.float32)
        for tap_row in range(3):
            for tap_col in range(3):
                total = total + jnp.einsum('oc,chw->ohw', kernel_f[tap_row, tap_col], rows[:, tap_row:tap_row + TH, tap_col:tap_col + width])
        mask_rows = lax.dynamic_slice_in_dim(land, (index * TH).astype(jnp.int32), TH, 0)
        return ((total + bias[:, None, None]) * mask_rows[None]).astype(jnp.bfloat16)

    bands = lax.map(band, jnp.arange(N_LAT, dtype=jnp.int32))
    return bands.transpose(1, 0, 2, 3).reshape(C, N_LAT * TH, width)
```

```python
import jax
import jax.numpy as jnp
from jax import lax
from jax.experimental import pallas as pl
from jax.experimental.pallas import tpu as pltpu
from jax.sharding import PartitionSpec as P

N_LAT = 8
N_LON = 16
DEVICES = N_LAT * N_LON
PR = 18
PC = 8
HELD = 960
HELD_COLS = 40
C_IN = 69
C = 64
MOST = 3
GROUP = 3
STEPS = PR // GROUP
BF16 = jnp.bfloat16
F32 = jnp.float32


def position():
    return lax.axis_index("lat"), lax.axis_index("lon")


def offsets(ids_ref):
    first = ids_ref[0, 0]
    owner = first // HELD
    local = first - owner * HELD
    row = local // HELD_COLS
    col = local - row * HELD_COLS
    return row * 8 + owner // N_LON, col * 16 + owner % N_LON


def iota(shape, dim):
    return lax.broadcasted_iota(jnp.int32, shape, dim)


def build_weights(w_ref, wide):
    wide[...] = jnp.zeros(wide.shape, F32)
    w = w_ref[...].astype(F32)
    for g in range(8):
        wide[g, 10 * g : 10 * g + C_IN, 0:C] = w
        wide[g, 10 * g + C_IN : 10 * g + 2 * C_IN, C : 2 * C] = w


def pack_blocks(ids_ref, coarse_ref, w_ref, send, wide, rows):
    a, b = position()
    r0, c0 = offsets(ids_ref)
    build_weights(w_ref, wide)
    first_row = (a - r0) & 7
    local_row = (r0 + first_row) >> 3
    first_col = (b - c0) & 15
    local_col = (c0 + first_col) >> 4
    count = DEVICES * MOST
    slot = iota((count, 128), 0)
    tile = (slot * 21846) >> 16
    place = slot - 3 * tile
    n = ((PR * (tile >> 4) + 6 - first_row) >> 3) + place
    n = jnp.clip(n, 0, PR - 1)
    m = jnp.clip((PC * (tile & 15) + PC - first_col) >> 4, 0, 7)
    col = local_col + m
    col = jnp.where(col >= HELD_COLS, col - HELD_COLS, col)
    which = (local_row + n) * HELD_COLS + col
    lane = iota((count, 128), 1)
    picks = [jnp.where(which - 128 * k == lane, 1.0, 0.0).astype(BF16) for k in range(8)]
    pick = jnp.concatenate(picks, axis=1)[:, :HELD]
    taken = jnp.dot(pick, coarse_ref[...], preferred_element_type=F32).astype(BF16)
    for g in range(8):
        width = min(256, 16 * C_IN - 128 * g)
        part = taken[:, 128 * g : 128 * g + width]
        rows[pl.ds(g, count, stride=8), :] = jnp.dot(
            part, wide[g, :width, :].astype(BF16), preferred_element_type=F32
        )
    send[...] = rows[...].reshape(count, 8, 128).astype(BF16)


def build_spread(interp_ref, spread):
    row = iota((48, 16), 0)
    cell = 2 * (row & 7) + jnp.where(row < 32, row >> 4, (row >> 3) & 1)
    choose = jnp.where(cell == iota((48, 16), 1), 1.0, 0.0).astype(BF16)
    source = jnp.dot(choose, interp_ref[...], preferred_element_type=F32).astype(BF16)
    lane = iota((1, 256), 1)
    fine = iota((256, 256), 0)
    row_id = iota((48, 256), 0)

    def body(index, carry):
        t = index >> 2
        slot = index & 3
        fy = 8 * t + 4 * (lane >> 7) + ((lane >> 5) & 3)
        over = jnp.where(fy == 15 * t, 15 - 15 * t, -1)
        from_y = jnp.where(slot == 3, over, fy + slot - 1)
        inside = (from_y >= 0) & (from_y <= 15)
        for dx in range(3):
            from_x = (lane & 31) + (dx - 1)
            target = jnp.where(inside, from_y * 16 + (from_x & 15), -1)
            hit = jnp.where(fine == target, 1.0, 0.0).astype(BF16)
            value = jnp.dot(source, hit, preferred_element_type=F32)
            outer = (-1, 9, 2)[dx]
            patch = jnp.where(row_id < 32, (row_id >> 3) & 1, outer)
            value = jnp.where(patch == (from_x >> 4), value, 0.0)
            for q in range(4):
                for v in range(2):
                    half = value[:, 128 * v : 128 * v + 128]
                    if q:
                        half = pltpu.roll(half, 32 * q, 1)
                    half = half.astype(BF16)
                    lanes = pl.ds(128 * v, 128)
                    start = pl.multiple_of(slot * 128 + 32 * dx, 32)
                    spread[t, q, pl.ds(start, 32), lanes] = half[:32]
                    if dx != 1:
                        start = pl.multiple_of(slot * 128 + 96 + 8 * dx, 16)
                        spread[t, q, pl.ds(start, 16), lanes] = half[32:]
        return carry

    lax.fori_loop(0, 8, body, 0)


def build_taps(kernel_ref, taps):
    taps[...] = jnp.zeros(taps.shape, BF16)
    for dy in range(3):
        for dx in range(3):
            taps[64 * dy : 64 * dy + 64, 64 * dx : 64 * dx + 64] = kernel_ref[dy, dx]


def prepare_kernel(ids_ref, coarse_ref, w_ref, interp_ref, kernel_ref, send, spread, taps, wide, rows):
    pack_blocks(ids_ref, coarse_ref, w_ref, send, wide, rows)
    build_spread(interp_ref, spread)
    build_taps(kernel_ref, taps)


def build_left(ids_ref, valid_ref, got, taps, left):
    lat, lon = position()
    r0, c0 = offsets(ids_ref)
    low = iota((8, 128), 1) < 64

    def body(row, carry):
        pr = row - 1
        u = PR * lat + pr
        holder = ((r0 + u) & 7) * N_LON
        start = (PR * lat + 6 - (u & 7)) >> 3
        place = (u >> 3) - start
        up = pr < 0
        down = pr >= PR
        near_lat = lat + jnp.where(up, -1, jnp.where(down, 1, 0))
        near_row = jnp.where(up, PR - 1, jnp.where(down, 0, pr))
        row_ok = (near_lat >= 0) & (near_lat < N_LAT)
        near_lat = jnp.clip(near_lat, 0, N_LAT - 1)
        blocks = []
        for col in range(PC + 2):
            pc = col - 1
            b = (c0 + PC * lon + pc) & 15
            near_lon = lon + (-1 if pc < 0 else 1 if pc >= PC else 0)
            ok = row_ok & (near_lon >= 0) & (near_lon < N_LON)
            near_lon = jnp.clip(near_lon, 0, N_LON - 1)
            live = valid_ref[near_lat * N_LON + near_lon, near_row * PC + pc % PC]
            live = jnp.where(ok, live, 0)
            block = got[(holder + b) * MOST + place].astype(F32)
            blocks.append(jnp.where(live > 0, block, 0.0))
        zero = jnp.zeros((8, 128), F32)
        keep = [jnp.where(low, x, 0.0) for x in blocks]
        keep_hi = [jnp.where(low, 0.0, x) for x in blocks]
        turned = [pltpu.roll(x, 64, 1) for x in keep_hi]
        turned_hi = [pltpu.roll(x, 64, 1) for x in keep]
        for pair in range(2):
            first, second = [], []
            for q in (2 * pair, 2 * pair + 1):
                j, k = 2 * q + 1, 2 * q + 2
                main = [keep[j], keep[k], turned[j], turned[k]]
                first += main
                first += [turned_hi[j], turned_hi[k], keep_hi[j], keep_hi[k]]
                first += [zero] * 4
                first += [keep[j - 1], turned[j - 1], zero, zero]
                second += [zero] * 8
                second += main
                second += [zero, zero, keep[k + 1], turned[k + 1]]
            right = jnp.concatenate(
                [
                    jnp.concatenate(first, axis=0).astype(BF16),
                    jnp.concatenate(second, axis=0).astype(BF16),
                ],
                axis=1,
            )
            value = lax.dot_general(
                taps[...], right, (((1,), (1,)), ((), ())), preferred_element_type=F32
            ).astype(BF16)
            start = pl.multiple_of(row * 64, 64)
            for side in range(2):
                for dy in range(3):
                    left[2 * pair + side, dy, pl.ds(start, 64), :] = value[
                        64 * dy : 64 * dy + 64, 128 * side : 128 * side + 128
                    ]
        return carry

    lax.fori_loop(0, PR + 2, body, 0)


def fine_kernel(ids_ref, valid_ref, got, spread, taps, bias_ref, out_ref, left, shift, stage):
    step = pl.program_id(0)

    @pl.when(step == 0)
    def _():
        build_left(ids_ref, valid_ref, got, taps, left)
        across = jnp.where(iota((64, 64), 0) == iota((64, 64), 1), bias_ref[...], 0.0)
        shift[...] = jnp.broadcast_to(jnp.sum(across, axis=1, keepdims=True), (64, 128))

    lat, lon = position()
    tile = lat * N_LON + lon
    size = GROUP * 64
    base = pl.multiple_of((GROUP * step + 1) * 64, 64)
    lane = iota((64, 128), 1) >> 4
    masks = []
    for r in range(GROUP):
        mask = jnp.zeros((64, 128), jnp.int32)
        for pc in range(PC):
            live = valid_ref[tile, (GROUP * step + r) * PC + pc]
            mask = jnp.where(lane == pc, live, mask)
        masks.append(mask > 0)
    land = jnp.concatenate(masks, axis=0)
    bias = jnp.concatenate([shift[...]] * GROUP, axis=0)
    quarter = iota((size, 128), 1) >> 5
    for t in range(2):
        parts = []
        for q in range(4):
            edge = left[q, 0, pl.ds(base - 64, size), :] if t == 0 else left[q, 2, pl.ds(base + 64, size), :]
            near = jnp.concatenate([left[q, 0, pl.ds(base, size), :], left[q, 1, pl.ds(base, size), :]], axis=1)
            far = jnp.concatenate([left[q, 2, pl.ds(base, size), :], edge], axis=1)
            parts.append(
                jnp.dot(near, spread[t, q, 0:256, :], preferred_element_type=F32)
                + jnp.dot(far, spread[t, q, 256:512, :], preferred_element_type=F32)
            )
        for v in range(2):
            for s in range(4):
                halves = [parts[(p - s) & 3][:, 128 * v : 128 * v + 128] for p in range(4)]
                value = jnp.where(quarter == 0, halves[0], jnp.where(quarter == 1, halves[1], jnp.where(quarter == 2, halves[2], halves[3])))
                if s:
                    value = pltpu.roll(value, 128 - 32 * s, 1)
                value = jnp.where(land, value + bias, 0.0)
                stage[pl.ds(8 * t + 4 * v + s, size, stride=16), :] = value
    for r in range(GROUP):
        block = stage[pl.ds(r * 1024, 1024), :].reshape(64, 16, 128)
        out_ref[:, 16 * r : 16 * r + 16, :] = block.astype(BF16)


def prepare(ids, coarse, w_mix, interp, kernel):
    vmem = pl.BlockSpec(memory_space=pltpu.VMEM)
    return pl.pallas_call(
        prepare_kernel,
        grid=(1,),
        out_shape=(
            jax.ShapeDtypeStruct((DEVICES * MOST, 8, 128), BF16),
            jax.ShapeDtypeStruct((2, 4, 512, 256), BF16),
            jax.ShapeDtypeStruct((192, 256), BF16),
        ),
        in_specs=[pl.BlockSpec((8, 128), lambda i: (0, 0), memory_space=pltpu.SMEM)] + [vmem] * 4,
        out_specs=(vmem, vmem, vmem),
        scratch_shapes=[
            pltpu.VMEM((8, 256, 128), F32),
            pltpu.VMEM((DEVICES * MOST * 8, 128), F32),
        ],
        name="prepare",
    )(ids, coarse, w_mix, interp, kernel)


def finish(ids, valid, got, spread, taps, bias):
    vmem = pl.BlockSpec(memory_space=pltpu.VMEM)
    return pl.pallas_call(
        fine_kernel,
        grid=(STEPS,),
        out_shape=jax.ShapeDtypeStruct((C, PR * 16, PC * 16), BF16),
        in_specs=[
            pl.BlockSpec((8, 128), lambda i: (0, 0), memory_space=pltpu.SMEM),
            pl.BlockSpec(memory_space=pltpu.SMEM),
            vmem,
            vmem,
            vmem,
            vmem,
        ],
        out_specs=pl.BlockSpec((C, GROUP * 16, PC * 16), lambda i: (0, i, 0)),
        scratch_shapes=[
            pltpu.VMEM((4, 3, (PR + 2) * 64, 128), BF16),
            pltpu.VMEM((64, 128), F32),
            pltpu.VMEM((GROUP * 64 * 16, 128), F32),
        ],
        name="finish",
    )(ids, valid, got, spread, taps, bias)


def per_device(coarse, w_mix, interp, kernel, bias, block_ids, valid):
    send, spread, taps = prepare(block_ids, coarse, w_mix, interp, kernel)
    got = lax.all_to_all(send, ("lat", "lon"), split_axis=0, concat_axis=0, tiled=True)
    return finish(block_ids, valid, got, spread, taps, bias.reshape(1, C))


def solution(mesh):
    placed = (P(("lat", "lon"), None), P(), P(), P(), P(), P(), P())
    return jax.shard_map(
        per_device, mesh=mesh, in_specs=placed, out_specs=P(None, "lat", "lon"), check_vma=False
    )
```

```python
import jax
import jax.numpy as jnp
from jax import lax
from jax.experimental import pallas as pl
from jax.experimental.pallas import tpu as pltpu
from jax.sharding import PartitionSpec as P

N_LAT = 8
N_LON = 16
DEVICES = N_LAT * N_LON
PR = 18
PC = 8
HELD = 960
HELD_COLS = 40
C_IN = 69
C = 64
MOST = 3
GROUP = 3
STEPS = PR // GROUP
MESH = pl.DeviceIdType.MESH
BF16 = jnp.bfloat16
F32 = jnp.float32


def position():
    return lax.axis_index("lat"), lax.axis_index("lon")


def offsets(ids_ref):
    first = ids_ref[0, 0]
    owner = first // HELD
    local = first - owner * HELD
    row = local // HELD_COLS
    col = local - row * HELD_COLS
    return row * 8 + owner // N_LON, col * 16 + owner % N_LON


def iota(shape, dim):
    return lax.broadcasted_iota(jnp.int32, shape, dim)


def build_weights(w_ref, wide):
    wide[...] = jnp.zeros(wide.shape, F32)
    w = jnp.transpose(w_ref[...].astype(F32))
    for g in range(8):
        wide[g, 10 * g : 10 * g + C_IN, 0:C] = w
        wide[g, 10 * g + C_IN : 10 * g + 2 * C_IN, C : 2 * C] = w


def pack_blocks(ids_ref, coarse_ref, w_ref, send, wide, rows):
    a, b = position()
    r0, c0 = offsets(ids_ref)
    build_weights(w_ref, wide)
    first_row = (a - r0) & 7
    local_row = (r0 + first_row) >> 3
    first_col = (b - c0) & 15
    local_col = (c0 + first_col) >> 4
    count = DEVICES * MOST
    slot = iota((count, 128), 0)
    tile = (slot * 21846) >> 16
    place = slot - 3 * tile
    n = ((PR * (tile >> 4) + 6 - first_row) >> 3) + place
    n = jnp.clip(n, 0, PR - 1)
    m = jnp.clip((PC * (tile & 15) + PC - first_col) >> 4, 0, 7)
    col = local_col + m
    col = jnp.where(col >= HELD_COLS, col - HELD_COLS, col)
    which = (local_row + n) * HELD_COLS + col
    lane = iota((count, 128), 1)
    picks = [jnp.where(which - 128 * k == lane, 1.0, 0.0).astype(BF16) for k in range(8)]
    pick = jnp.concatenate(picks, axis=1)[:, :HELD]
    taken = jnp.dot(pick, coarse_ref[...], preferred_element_type=F32).astype(BF16)
    for g in range(8):
        width = min(256, 16 * C_IN - 128 * g)
        part = taken[:, 128 * g : 128 * g + width]
        rows[pl.ds(g, count, stride=8), :] = jnp.dot(
            part, wide[g, :width, :].astype(BF16), preferred_element_type=F32
        )
    send[...] = rows[...].reshape(DEVICES, MOST, 8, 128).astype(BF16)


def build_spread(interp_ref, spread):
    row = iota((48, 16), 0)
    cell = 2 * (row & 7) + jnp.where(row < 32, row >> 4, (row >> 3) & 1)
    choose = jnp.where(cell == iota((48, 16), 1), 1.0, 0.0).astype(BF16)
    source = jnp.dot(choose, interp_ref[...], preferred_element_type=F32).astype(BF16)
    lane = iota((1, 256), 1)
    fine = iota((256, 256), 0)
    row_id = iota((48, 256), 0)

    def body(index, carry):
        t = index >> 2
        slot = index & 3
        fy = 8 * t + 4 * (lane >> 7) + ((lane >> 5) & 3)
        over = jnp.where(fy == 15 * t, 15 - 15 * t, -1)
        from_y = jnp.where(slot == 3, over, fy + slot - 1)
        inside = (from_y >= 0) & (from_y <= 15)
        for dx in range(3):
            from_x = (lane & 31) + (dx - 1)
            target = jnp.where(inside, from_y * 16 + (from_x & 15), -1)
            hit = jnp.where(fine == target, 1.0, 0.0).astype(BF16)
            value = jnp.dot(source, hit, preferred_element_type=F32)
            outer = (-1, 9, 2)[dx]
            patch = jnp.where(row_id < 32, (row_id >> 3) & 1, outer)
            value = jnp.where(patch == (from_x >> 4), value, 0.0)
            for q in range(4):
                for v in range(2):
                    half = value[:, 128 * v : 128 * v + 128]
                    if q:
                        half = pltpu.roll(half, 32 * q, 1)
                    half = half.astype(BF16)
                    lanes = pl.ds(128 * v, 128)
                    start = pl.multiple_of(slot * 128 + 32 * dx, 32)
                    spread[t, q, pl.ds(start, 32), lanes] = half[:32]
                    if dx != 1:
                        start = pl.multiple_of(slot * 128 + 96 + 8 * dx, 16)
                        spread[t, q, pl.ds(start, 16), lanes] = half[32:]
        return carry

    lax.fori_loop(0, 8, body, 0)


def build_taps(kernel_ref, taps):
    taps[...] = jnp.zeros(taps.shape, BF16)
    for dy in range(3):
        for dx in range(3):
            taps[64 * dy : 64 * dy + 64, 64 * dx : 64 * dx + 64] = kernel_ref[dy, dx]


def peer(me, k):
    other = lax.rem(me + k, DEVICES)
    return other, (lax.div(other, N_LON), lax.rem(other, N_LON))


def exchange_kernel(
    ids_ref, coarse_ref, w_ref, interp_ref, kernel_ref, got, spread, taps, wide, rows, send, send_sem, got_sem
):
    lat, lon = position()
    me = lat * N_LON + lon
    barrier = pltpu.get_barrier_semaphore()

    def greet(k, carry):
        pl.semaphore_signal(barrier, inc=1, device_id=peer(me, k)[1], device_id_type=MESH)
        return carry

    lax.fori_loop(1, DEVICES, greet, 0)
    pack_blocks(ids_ref, coarse_ref, w_ref, send, wide, rows)
    pl.semaphore_wait(barrier, DEVICES - 1)

    def push(k, carry):
        other, where = peer(me, k)
        pltpu.make_async_remote_copy(
            src_ref=send.at[other],
            dst_ref=got.at[me],
            send_sem=send_sem,
            recv_sem=got_sem,
            device_id=where,
            device_id_type=MESH,
        ).start()
        return carry

    lax.fori_loop(1, DEVICES, push, 0)
    got[me] = send[me]
    build_spread(interp_ref, spread)
    build_taps(kernel_ref, taps)
    others = pl.ds(0, DEVICES - 1)
    pltpu.make_async_copy(send.at[others], got.at[others], got_sem).wait()
    pltpu.make_async_copy(send.at[others], got.at[others], send_sem).wait()


def build_left(ids_ref, valid_ref, got, taps, left):
    lat, lon = position()
    r0, c0 = offsets(ids_ref)
    low = iota((8, 128), 1) < 64

    def body(row, carry):
        pr = row - 1
        u = PR * lat + pr
        holder = ((r0 + u) & 7) * N_LON
        start = (PR * lat + 6 - (u & 7)) >> 3
        place = (u >> 3) - start
        up = pr < 0
        down = pr >= PR
        near_lat = lat + jnp.where(up, -1, jnp.where(down, 1, 0))
        near_row = jnp.where(up, PR - 1, jnp.where(down, 0, pr))
        row_ok = (near_lat >= 0) & (near_lat < N_LAT)
        near_lat = jnp.clip(near_lat, 0, N_LAT - 1)
        blocks = []
        for col in range(PC + 2):
            pc = col - 1
            b = (c0 + PC * lon + pc) & 15
            near_lon = lon + (-1 if pc < 0 else 1 if pc >= PC else 0)
            ok = row_ok & (near_lon >= 0) & (near_lon < N_LON)
            near_lon = jnp.clip(near_lon, 0, N_LON - 1)
            live = valid_ref[near_row * PC + pc % PC, near_lat * N_LON + near_lon]
            live = jnp.where(ok, live, 0)
            block = got[holder + b, place].astype(F32)
            blocks.append(jnp.where(live > 0, block, 0.0))
        zero = jnp.zeros((8, 128), F32)
        keep = [jnp.where(low, x, 0.0) for x in blocks]
        keep_hi = [jnp.where(low, 0.0, x) for x in blocks]
        turned = [pltpu.roll(x, 64, 1) for x in keep_hi]
        turned_hi = [pltpu.roll(x, 64, 1) for x in keep]
        for pair in range(2):
            first, second = [], []
            for q in (2 * pair, 2 * pair + 1):
                j, k = 2 * q + 1, 2 * q + 2
                main = [keep[j], keep[k], turned[j], turned[k]]
                first += main
                first += [turned_hi[j], turned_hi[k], keep_hi[j], keep_hi[k]]
                first += [zero] * 4
                first += [keep[j - 1], turned[j - 1], zero, zero]
                second += [zero] * 8
                second += main
                second += [zero, zero, keep[k + 1], turned[k + 1]]
            right = jnp.concatenate(
                [
                    jnp.concatenate(first, axis=0).astype(BF16),
                    jnp.concatenate(second, axis=0).astype(BF16),
                ],
                axis=1,
            )
            value = lax.dot_general(
                taps[...], right, (((1,), (1,)), ((), ())), preferred_element_type=F32
            ).astype(BF16)
            start = pl.multiple_of(row * 64, 64)
            for side in range(2):
                for dy in range(3):
                    left[2 * pair + side, dy, pl.ds(start, 64), :] = value[
                        64 * dy : 64 * dy + 64, 128 * side : 128 * side + 128
                    ]
        return carry

    lax.fori_loop(0, PR + 2, body, 0)


def fine_kernel(ids_ref, valid_ref, got, spread, taps, bias_ref, out_ref, left, shift, stage):
    step = pl.program_id(0)

    @pl.when(step == 0)
    def _():
        build_left(ids_ref, valid_ref, got, taps, left)
        across = jnp.where(iota((64, 64), 0) == iota((64, 64), 1), bias_ref[...], 0.0)
        shift[...] = jnp.broadcast_to(jnp.sum(across, axis=1, keepdims=True), (64, 128))

    lat, lon = position()
    tile = lat * N_LON + lon
    size = GROUP * 64
    base = pl.multiple_of((GROUP * step + 1) * 64, 64)
    lane = iota((64, 128), 1) >> 4
    masks = []
    for r in range(GROUP):
        mask = jnp.zeros((64, 128), jnp.int32)
        for pc in range(PC):
            live = valid_ref[(GROUP * step + r) * PC + pc, tile]
            mask = jnp.where(lane == pc, live, mask)
        masks.append(mask > 0)
    land = jnp.concatenate(masks, axis=0)
    bias = jnp.concatenate([shift[...]] * GROUP, axis=0)
    quarter = iota((size, 128), 1) >> 5
    for t in range(2):
        parts = []
        for q in range(4):
            edge = left[q, 0, pl.ds(base - 64, size), :] if t == 0 else left[q, 2, pl.ds(base + 64, size), :]
            near = jnp.concatenate([left[q, 0, pl.ds(base, size), :], left[q, 1, pl.ds(base, size), :]], axis=1)
            far = jnp.concatenate([left[q, 2, pl.ds(base, size), :], edge], axis=1)
            parts.append(
                jnp.dot(near, spread[t, q, 0:256, :], preferred_element_type=F32)
                + jnp.dot(far, spread[t, q, 256:512, :], preferred_element_type=F32)
            )
        for v in range(2):
            for s in range(4):
                halves = [parts[(p - s) & 3][:, 128 * v : 128 * v + 128] for p in range(4)]
                value = jnp.where(quarter == 0, halves[0], jnp.where(quarter == 1, halves[1], jnp.where(quarter == 2, halves[2], halves[3])))
                if s:
                    value = pltpu.roll(value, 128 - 32 * s, 1)
                value = jnp.where(land, value + bias, 0.0)
                stage[pl.ds(8 * t + 4 * v + s, size, stride=16), :] = value
    for r in range(GROUP):
        block = stage[pl.ds(r * 1024, 1024), :].reshape(64, 16, 128)
        out_ref[:, 16 * r : 16 * r + 16, :] = block.astype(BF16)


def exchange(ids, coarse, w_mix, interp, kernel):
    vmem = pl.BlockSpec(memory_space=pltpu.VMEM)
    return pl.pallas_call(
        exchange_kernel,
        grid=(1,),
        out_shape=(
            jax.ShapeDtypeStruct((DEVICES, MOST, 8, 128), BF16),
            jax.ShapeDtypeStruct((2, 4, 512, 256), BF16),
            jax.ShapeDtypeStruct((192, 256), BF16),
        ),
        in_specs=[pl.BlockSpec((8, 128), lambda i: (0, 0), memory_space=pltpu.SMEM)] + [vmem] * 4,
        out_specs=(vmem, vmem, vmem),
        scratch_shapes=[
            pltpu.VMEM((8, 256, 128), F32),
            pltpu.VMEM((DEVICES * MOST * 8, 128), F32),
            pltpu.VMEM((DEVICES, MOST, 8, 128), BF16),
            pltpu.SemaphoreType.DMA,
            pltpu.SemaphoreType.DMA,
        ],
        compiler_params=pltpu.CompilerParams(collective_id=0, has_side_effects=True),
        name="exchange",
    )(ids, coarse, w_mix, interp, kernel)


def finish(ids, valid, got, spread, taps, bias):
    vmem = pl.BlockSpec(memory_space=pltpu.VMEM)
    return pl.pallas_call(
        fine_kernel,
        grid=(STEPS,),
        out_shape=jax.ShapeDtypeStruct((C, PR * 16, PC * 16), BF16),
        in_specs=[
            pl.BlockSpec((8, 128), lambda i: (0, 0), memory_space=pltpu.SMEM),
            pl.BlockSpec(memory_space=pltpu.SMEM),
            vmem,
            vmem,
            vmem,
            vmem,
        ],
        out_specs=pl.BlockSpec((C, GROUP * 16, PC * 16), lambda i: (0, i, 0)),
        scratch_shapes=[
            pltpu.VMEM((4, 3, (PR + 2) * 64, 128), BF16),
            pltpu.VMEM((64, 128), F32),
            pltpu.VMEM((GROUP * 64 * 16, 128), F32),
        ],
        name="finish",
    )(ids, valid, got, spread, taps, bias)


def per_device(coarse, w_mix, interp, kernel, bias, block_ids, valid):
    ids, live = block_ids.T, valid.T
    got, spread, taps = exchange(ids, coarse, w_mix.T, interp, kernel)
    return finish(ids, live, got, spread, taps, bias.reshape(1, C))


def solution(mesh):
    placed = (P(("lat", "lon"), None), P(), P(), P(), P(), P(), P())
    return jax.shard_map(
        per_device, mesh=mesh, in_specs=placed, out_specs=P(None, "lat", "lon"), check_vma=False
    )
```

```python
import jax
import jax.numpy as jnp
from jax import lax
from jax.experimental import pallas as pl
from jax.experimental.pallas import tpu as pltpu
from jax.sharding import PartitionSpec as P

N_LAT = 8
N_LON = 16
DEVICES = N_LAT * N_LON
PR = 18
PC = 8
HELD = 960
HELD_COLS = 40
C_IN = 69
C = 64
MOST = 3
GROUP = 6
EARLY = 2 * 6 * 16
PITCH = GROUP * 64 + 8
PARTS = 1
BATCH = GROUP * PARTS
LEFT = (4, 3, (PR + 2) * 64, 128)
MESH = pl.DeviceIdType.MESH
BF16 = jnp.bfloat16
F32 = jnp.float32


def position():
    return lax.axis_index("lat"), lax.axis_index("lon")


def offsets(ids_ref):
    first = ids_ref[0, 0]
    owner = first // HELD
    local = first - owner * HELD
    row = local // HELD_COLS
    col = local - row * HELD_COLS
    return row * 8 + owner // N_LON, col * 16 + owner % N_LON


def iota(shape, dim):
    return lax.broadcasted_iota(jnp.int32, shape, dim)


def build_weights(w_ref, wide):
    wide[...] = jnp.zeros(wide.shape, F32)
    w = jnp.transpose(w_ref[...].astype(F32))
    for g in range(8):
        wide[g, 10 * g : 10 * g + C_IN, 0:C] = w
        wide[g, 10 * g + C_IN : 10 * g + 2 * C_IN, C : 2 * C] = w


def pack_blocks(ids_ref, coarse, wide, rows, send):
    a, b = position()
    r0, c0 = offsets(ids_ref)
    first_row = (a - r0) & 7
    local_row = (r0 + first_row) >> 3
    first_col = (b - c0) & 15
    local_col = (c0 + first_col) >> 4
    count = DEVICES * MOST
    slot = iota((count, 128), 0)
    tile = slot & (DEVICES - 1)
    n = ((PR * (tile >> 4) + 6 - first_row) >> 3) + (slot >> 7)
    n = jnp.clip(n, 0, PR - 1)
    m = jnp.clip((PC * (tile & 15) + PC - first_col) >> 4, 0, 7)
    col = local_col + m
    col = jnp.where(col >= HELD_COLS, col - HELD_COLS, col)
    which = (local_row + n) * HELD_COLS + col
    lane = iota((count, 128), 1)
    picks = [jnp.where(which - 128 * k == lane, 1.0, 0.0).astype(BF16) for k in range(8)]
    pick = jnp.concatenate(picks, axis=1)[:, :HELD]
    taken = jnp.dot(pick, coarse[...], preferred_element_type=F32).astype(BF16)
    for g in range(8):
        width = min(256, 16 * C_IN - 128 * g)
        part = taken[:, 128 * g : 128 * g + width]
        rows[pl.ds(g, count, stride=8), :] = jnp.dot(
            part, wide[g, :width, :].astype(BF16), preferred_element_type=F32
        )
    send[...] = rows[...].reshape(MOST, DEVICES, 8, 128).astype(BF16)


def build_spread(interp_ref, spread):
    row = iota((48, 16), 0)
    cell = 2 * (row & 7) + jnp.where(row < 32, row >> 4, (row >> 3) & 1)
    choose = jnp.where(cell == iota((48, 16), 1), 1.0, 0.0).astype(BF16)
    source = jnp.dot(choose, interp_ref[...], preferred_element_type=F32).astype(BF16)
    lane = iota((1, 256), 1)
    fine = iota((256, 256), 0)
    row_id = iota((48, 256), 0)

    def body(index, carry):
        t = index >> 2
        slot = index & 3
        fy = 8 * t + 4 * (lane >> 7) + ((lane >> 5) & 3)
        over = jnp.where(fy == 15 * t, 15 - 15 * t, -1)
        from_y = jnp.where(slot == 3, over, fy + slot - 1)
        inside = (from_y >= 0) & (from_y <= 15)
        for dx in range(3):
            from_x = (lane & 31) + (dx - 1)
            target = jnp.where(inside, from_y * 16 + (from_x & 15), -1)
            hit = jnp.where(fine == target, 1.0, 0.0).astype(BF16)
            value = jnp.dot(source, hit, preferred_element_type=F32)
            outer = (-1, 9, 2)[dx]
            patch = jnp.where(row_id < 32, (row_id >> 3) & 1, outer)
            value = jnp.where(patch == (from_x >> 4), value, 0.0)
            for q in range(4):
                for v in range(2):
                    half = value[:, 128 * v : 128 * v + 128]
                    if q:
                        half = pltpu.roll(half, 32 * q, 1)
                    half = half.astype(BF16)
                    lanes = pl.ds(128 * v, 128)
                    start = pl.multiple_of(slot * 128 + 32 * dx, 32)
                    spread[t, q, pl.ds(start, 32), lanes] = half[:32]
                    if dx != 1:
                        start = pl.multiple_of(slot * 128 + 96 + 8 * dx, 16)
                        spread[t, q, pl.ds(start, 16), lanes] = half[32:]
        return carry

    lax.fori_loop(0, 8, body, 0)


def build_taps(kernel_ref, taps):
    taps[...] = jnp.zeros(taps.shape, BF16)
    for dy in range(3):
        for dx in range(3):
            taps[64 * dy : 64 * dy + 64, 64 * dx : 64 * dx + 64] = kernel_ref[dy, dx]


def far_first():
    def hops(step):
        return sum(min(d, 4 - d) for d in step[:3])

    steps = [(y, z, x, c) for y in range(4) for z in range(4) for x in range(4) for c in range(2)]
    return sorted(steps[1:], key=hops, reverse=True)


def peers():
    lat, lon = position()
    ys = [lax.rem(lax.div(lat, 2) + d, 4) * 2 for d in range(4)]
    cs = [lax.rem(lat + d, 2) for d in range(2)]
    zs = [lax.rem(lax.div(lon, 4) + d, 4) * 4 for d in range(4)]
    xs = [lax.rem(lon + d, 4) for d in range(4)]
    return [(ys[y] + cs[c], zs[z] + xs[x]) for y, z, x, c in far_first()]


def build_left(ids_ref, valid_ref, got, taps, left, first_row, last_row):
    lat, lon = position()
    r0, c0 = offsets(ids_ref)
    low = iota((8, 128), 1) < 64

    def pair_of_rows(index, carry):
        one_row(first_row + 2 * index)
        one_row(first_row + 2 * index + 1)
        return carry

    def one_row(row):
        pr = row - 1
        u = PR * lat + pr
        holder = ((r0 + u) & 7) * N_LON
        up = pr < 0
        down = pr >= PR
        near_lat = lat + jnp.where(up, -1, jnp.where(down, 1, 0))
        near_row = jnp.where(up, PR - 1, jnp.where(down, 0, pr))
        row_ok = (near_lat >= 0) & (near_lat < N_LAT)
        near_lat = jnp.clip(near_lat, 0, N_LAT - 1)
        blocks = []
        for col in range(PC + 2):
            pc = col - 1
            b = (c0 + PC * lon + pc) & 15
            near_lon = lon + (-1 if pc < 0 else 1 if pc >= PC else 0)
            ok = row_ok & (near_lon >= 0) & (near_lon < N_LON)
            near_lon = jnp.clip(near_lon, 0, N_LON - 1)
            live = valid_ref[near_row * PC + pc % PC, near_lat * N_LON + near_lon]
            live = jnp.where(ok, live, 0)
            block = got[holder + b].astype(F32)
            blocks.append(jnp.where(live > 0, block, 0.0))
        zero = jnp.zeros((8, 128), F32)
        keep = [jnp.where(low, x, 0.0) for x in blocks]
        keep_hi = [jnp.where(low, 0.0, x) for x in blocks]
        turned = [pltpu.roll(x, 64, 1) for x in keep_hi]
        turned_hi = [pltpu.roll(x, 64, 1) for x in keep]
        for pair in range(2):
            first, second = [], []
            for q in (2 * pair, 2 * pair + 1):
                j, k = 2 * q + 1, 2 * q + 2
                main = [keep[j], keep[k], turned[j], turned[k]]
                first += main
                first += [turned_hi[j], turned_hi[k], keep_hi[j], keep_hi[k]]
                first += [zero] * 4
                first += [keep[j - 1], turned[j - 1], zero, zero]
                second += [zero] * 8
                second += main
                second += [zero, zero, keep[k + 1], turned[k + 1]]
            right = jnp.concatenate(
                [
                    jnp.concatenate(first, axis=0).astype(BF16),
                    jnp.concatenate(second, axis=0).astype(BF16),
                ],
                axis=1,
            )
            value = lax.dot_general(
                taps[...], right, (((1,), (1,)), ((), ())), preferred_element_type=F32
            ).astype(BF16)
            start = pl.multiple_of(row * 64, 64)
            for side in range(2):
                for dy in range(3):
                    left[2 * pair + side, dy, pl.ds(start, 64), :] = value[
                        64 * dy : 64 * dy + 64, 128 * side : 128 * side + 128
                    ]

    lax.fori_loop(0, (last_row - first_row) // 2, pair_of_rows, 0)


def build_shift(bias_ref, shift):
    across = jnp.where(iota((C, C), 0) == iota((C, C), 1), bias_ref[...], 0.0)
    shift[...] = jnp.broadcast_to(jnp.sum(across, axis=1, keepdims=True), (C, 128))


def build_land(valid_ref, land):
    lat, lon = position()
    tile = lat * N_LON + lon
    lane = iota((8, 128), 1) >> 4

    def body(row, carry):
        mask = jnp.zeros((8, 128), jnp.int32)
        for pc in range(PC):
            mask = jnp.where(lane == pc, valid_ref[row * PC + pc, tile], mask)
        land[row] = mask
        return carry

    lax.fori_loop(0, PR, body, 0)


def fine_rows(first, land, left, spread, shift, stages, out):
    size = GROUP * 64
    quarter = iota((size, 128), 1) >> 5
    bias = jnp.concatenate([shift[...]] * GROUP, axis=0)
    for part, stage in enumerate(stages):
        top = first + part * GROUP
        base = pl.multiple_of((top + 1) * 64, 64)
        keep = [jnp.concatenate([land[top + r]] * 8, axis=0) for r in range(GROUP)]
        keep = jnp.concatenate(keep, axis=0) > 0
        for t in range(2):
            parts = []
            for q in range(4):
                lhs = [left[q, dy, pl.ds(base, size), :] for dy in range(3)]
                if t == 0:
                    lhs.append(left[q, 0, pl.ds(base - 64, size), :])
                else:
                    lhs.append(left[q, 2, pl.ds(base + 64, size), :])
                lhs = jnp.concatenate(lhs, axis=1)
                parts.append(jnp.dot(lhs, spread[t, q], preferred_element_type=F32))
            for v in range(2):
                for s in range(4):
                    cut = [parts[(p - s) & 3][:, 128 * v : 128 * v + 128] for p in range(4)]
                    value = cut[3]
                    for p in (2, 1, 0):
                        value = jnp.where(quarter == p, cut[p], value)
                    if s:
                        value = pltpu.roll(value, 128 - 32 * s, 1)
                    value = jnp.where(keep, value + bias, 0.0)
                    stage[pl.ds((8 * t + 4 * v + s) * PITCH, size), :] = value
        for r in range(GROUP):
            for o in range(C):
                block = stage[pl.ds(64 * r + o, 16, stride=PITCH), :]
                row = 16 * (part * GROUP + r)
                out[o, row : row + 16, :] = block.astype(BF16)


def exchange_kernel(
    ids_ref, valid_ref, coarse_ref, w_ref, interp_ref, kernel_ref, bias_ref,
    left, spread, early, shift, land,
    coarse, wide, rows, send, got_first, got_next, got_last, taps, stage, load_sem, send_sem, got_sem,
):
    lat, lon = position()
    me = lat * N_LON + lon
    load = pltpu.make_async_copy(coarse_ref, coarse, load_sem)
    load.start()
    barrier = pltpu.get_barrier_semaphore()

    targets = peers()
    for where in targets:
        pl.semaphore_signal(barrier, inc=1, device_id=where, device_id_type=MESH)
    build_weights(w_ref, wide)
    build_taps(kernel_ref, taps)
    build_shift(bias_ref, shift)
    build_land(valid_ref, land)
    load.wait()
    pack_blocks(ids_ref, coarse, wide, rows, send)
    pl.semaphore_wait(barrier, DEVICES - 1)
    got = (got_first, got_next, got_last)
    for s in range(MOST):
        for where in targets:
            pltpu.make_async_remote_copy(
                src_ref=send.at[s, where[0] * N_LON + where[1]],
                dst_ref=got[s].at[me],
                send_sem=send_sem,
                recv_sem=got_sem.at[s],
                device_id=where,
                device_id_type=MESH,
            ).start()
        got[s][me] = send[s, me]
    build_spread(interp_ref, spread)
    others = pl.ds(0, DEVICES - 1)
    for s in range(MOST):
        pltpu.make_async_copy(send.at[s, others], got[s].at[others], got_sem.at[s]).wait()
        build_left(ids_ref, valid_ref, got[s], taps, left, 8 * s, min(8 * s + 8, PR + 2))
        if s < MOST - 1:
            rows_out = pl.ds(BATCH * 16 * s, BATCH * 16)
            stages = [stage.at[part] for part in range(PARTS)]
            fine_rows(BATCH * s, land, left, spread, shift, stages, early.at[:, rows_out, :])
    for s in range(MOST):
        pltpu.make_async_copy(send.at[s, others], got[s].at[others], send_sem).wait()


def finish_kernel(left, spread, early, shift, land, out, stage, late, early_sem, late_sem):
    head = pltpu.make_async_copy(early, out.at[:, pl.ds(0, EARLY), :], early_sem)
    head.start()
    tails = []
    for part in range(PARTS):
        first = 2 * BATCH + GROUP * part
        fine_rows(first, land, left, spread, shift, [stage.at[part]], late.at[part])
        where = pl.ds(16 * first, 16 * GROUP)
        tail = pltpu.make_async_copy(late.at[part], out.at[:, where, :], late_sem.at[part])
        tail.start()
        tails.append(tail)
    head.wait()
    for tail in tails:
        tail.wait()


def exchange(ids, valid, coarse, w_mix, interp, kernel, bias):
    vmem = pl.BlockSpec(memory_space=pltpu.VMEM)
    smem = pl.BlockSpec(memory_space=pltpu.SMEM)
    slots = (DEVICES, 8, 128)
    return pl.pallas_call(
        exchange_kernel,
        grid=(1,),
        out_shape=(
            pltpu.VMEM(LEFT, BF16),
            pltpu.VMEM((2, 4, 512, 256), BF16),
            pltpu.VMEM((C, EARLY, 128), BF16),
            pltpu.VMEM((C, 128), F32),
            pltpu.VMEM((PR, 8, 128), jnp.int32),
        ),
        in_specs=[
            pl.BlockSpec((8, 128), lambda i: (0, 0), memory_space=pltpu.SMEM),
            smem,
            pl.BlockSpec(memory_space=pl.ANY),
            vmem,
            vmem,
            vmem,
            vmem,
        ],
        out_specs=(vmem,) * 5,
        scratch_shapes=[
            pltpu.VMEM((HELD, 16 * C_IN), BF16),
            pltpu.VMEM((8, 256, 128), F32),
            pltpu.VMEM((DEVICES * MOST * 8, 128), F32),
            pltpu.VMEM((MOST,) + slots, BF16),
            pltpu.VMEM(slots, BF16),
            pltpu.VMEM(slots, BF16),
            pltpu.VMEM(slots, BF16),
            pltpu.VMEM((192, 256), BF16),
            pltpu.VMEM((PARTS, 16 * PITCH, 128), F32),
            pltpu.SemaphoreType.DMA,
            pltpu.SemaphoreType.DMA,
            pltpu.SemaphoreType.DMA((MOST,)),
        ],
        compiler_params=pltpu.CompilerParams(
            collective_id=0, has_side_effects=True, vmem_limit_bytes=54 * 2**20
        ),
        name="exchange",
    )(ids, valid, coarse, w_mix, interp, kernel, bias)


def finish(*arrays):
    vmem = pl.BlockSpec(memory_space=pltpu.VMEM)
    return pl.pallas_call(
        finish_kernel,
        grid=(1,),
        out_shape=jax.ShapeDtypeStruct((C, PR * 16, PC * 16), BF16),
        in_specs=[vmem] * 5,
        out_specs=pl.BlockSpec(memory_space=pl.ANY),
        scratch_shapes=[
            pltpu.VMEM((PARTS, 16 * PITCH, 128), F32),
            pltpu.VMEM((PARTS, C, GROUP * 16, 128), BF16),
            pltpu.SemaphoreType.DMA,
            pltpu.SemaphoreType.DMA((PARTS,)),
        ],
        compiler_params=pltpu.CompilerParams(vmem_limit_bytes=30 * 2**20),
        name="finish",
    )(*arrays)


def per_device(coarse, w_mix, interp, kernel, bias, block_ids, valid):
    stay = [block_ids.T, valid.T, bias.reshape(1, C)]
    ids, live, bias = [pltpu.with_memory_space_constraint(x, pltpu.HBM) for x in stay]
    arrived = exchange(ids, live, coarse, w_mix.T, interp, kernel, bias)
    return finish(*arrived)


def solution(mesh):
    placed = (P(("lat", "lon"), None), P(), P(), P(), P(), P(), P())
    return jax.shard_map(
        per_device, mesh=mesh, in_specs=placed, out_specs=P(None, "lat", "lon"), check_vma=False
    )
```

```python
import jax
import jax.numpy as jnp
from jax import lax
from jax.experimental import pallas as pl
from jax.experimental.pallas import tpu as pltpu
from jax.sharding import PartitionSpec as P

N_LAT = 8
N_LON = 16
DEVICES = N_LAT * N_LON
PR = 18
PC = 8
HELD = 960
HELD_COLS = 40
C_IN = 69
C = 64
MOST = 3
GROUP = 6
EARLY = 2 * 6 * 16
PITCH = GROUP * 64 + 8
PARTS = 1
UNROLL = 4
BATCH = GROUP * PARTS
LEFT = (4, 3, (PR + 2) * 64, 128)
MESH = pl.DeviceIdType.MESH
BF16 = jnp.bfloat16
F32 = jnp.float32


def position():
    return lax.axis_index("lat"), lax.axis_index("lon")


def offsets(ids_ref):
    first = ids_ref[0, 0]
    owner = first // HELD
    local = first - owner * HELD
    row = local // HELD_COLS
    col = local - row * HELD_COLS
    return row * 8 + owner // N_LON, col * 16 + owner % N_LON


def iota(shape, dim):
    return lax.broadcasted_iota(jnp.int32, shape, dim)


def build_weights(w_ref, wide):
    wide[...] = jnp.zeros(wide.shape, F32)
    w = jnp.transpose(w_ref[...].astype(F32))
    for g in range(8):
        wide[g, 10 * g : 10 * g + C_IN, 0:C] = w
        wide[g, 10 * g + C_IN : 10 * g + 2 * C_IN, C : 2 * C] = w


def pack_blocks(ids_ref, coarse, wide, rows, send):
    a, b = position()
    r0, c0 = offsets(ids_ref)
    first_row = (a - r0) & 7
    local_row = (r0 + first_row) >> 3
    first_col = (b - c0) & 15
    local_col = (c0 + first_col) >> 4
    count = DEVICES * MOST
    slot = iota((count, 128), 0)
    tile = slot & (DEVICES - 1)
    n = ((PR * (tile >> 4) + 6 - first_row) >> 3) + (slot >> 7)
    n = jnp.clip(n, 0, PR - 1)
    m = jnp.clip((PC * (tile & 15) + PC - first_col) >> 4, 0, 7)
    col = local_col + m
    col = jnp.where(col >= HELD_COLS, col - HELD_COLS, col)
    which = (local_row + n) * HELD_COLS + col
    lane = iota((count, 128), 1)
    picks = [jnp.where(which - 128 * k == lane, 1.0, 0.0).astype(BF16) for k in range(8)]
    pick = jnp.concatenate(picks, axis=1)[:, :HELD]
    taken = jnp.dot(pick, coarse[...], preferred_element_type=F32).astype(BF16)
    for g in range(8):
        width = min(256, 16 * C_IN - 128 * g)
        part = taken[:, 128 * g : 128 * g + width]
        rows[pl.ds(g, count, stride=8), :] = jnp.dot(
            part, wide[g, :width, :].astype(BF16), preferred_element_type=F32
        )
    send[...] = rows[...].reshape(MOST, DEVICES, 8, 128).astype(BF16)


def build_spread(interp_ref, spread):
    row = iota((48, 16), 0)
    cell = 2 * (row & 7) + jnp.where(row < 32, row >> 4, (row >> 3) & 1)
    choose = jnp.where(cell == iota((48, 16), 1), 1.0, 0.0).astype(BF16)
    source = jnp.dot(choose, interp_ref[...], preferred_element_type=F32).astype(BF16)
    lane = iota((1, 256), 1)
    fine = iota((256, 256), 0)
    row_id = iota((48, 256), 0)

    def body(index, carry):
        t = index >> 2
        slot = index & 3
        fy = 8 * t + 4 * (lane >> 7) + ((lane >> 5) & 3)
        over = jnp.where(fy == 15 * t, 15 - 15 * t, -1)
        from_y = jnp.where(slot == 3, over, fy + slot - 1)
        inside = (from_y >= 0) & (from_y <= 15)
        for dx in range(3):
            from_x = (lane & 31) + (dx - 1)
            target = jnp.where(inside, from_y * 16 + (from_x & 15), -1)
            hit = jnp.where(fine == target, 1.0, 0.0).astype(BF16)
            value = jnp.dot(source, hit, preferred_element_type=F32)
            outer = (-1, 9, 2)[dx]
            patch = jnp.where(row_id < 32, (row_id >> 3) & 1, outer)
            value = jnp.where(patch == (from_x >> 4), value, 0.0)
            for q in range(4):
                for v in range(2):
                    half = value[:, 128 * v : 128 * v + 128]
                    if q:
                        half = pltpu.roll(half, 32 * q, 1)
                    half = half.astype(BF16)
                    lanes = pl.ds(128 * v, 128)
                    start = pl.multiple_of(slot * 128 + 32 * dx, 32)
                    spread[t, q, pl.ds(start, 32), lanes] = half[:32]
                    if dx != 1:
                        start = pl.multiple_of(slot * 128 + 96 + 8 * dx, 16)
                        spread[t, q, pl.ds(start, 16), lanes] = half[32:]
        return carry

    lax.fori_loop(0, 8, body, 0)


def build_taps(kernel_ref, taps):
    taps[...] = jnp.zeros(taps.shape, BF16)
    for dy in range(3):
        for dx in range(3):
            taps[64 * dy : 64 * dy + 64, 64 * dx : 64 * dx + 64] = kernel_ref[dy, dx]


def far_first():
    def hops(step):
        return sum(min(d, 4 - d) for d in step[:3])

    steps = [(y, z, x, c) for y in range(4) for z in range(4) for x in range(4) for c in range(2)]
    return sorted(steps[1:], key=hops, reverse=True)


def peers():
    lat, lon = position()
    ys = [lax.rem(lax.div(lat, 2) + d, 4) * 2 for d in range(4)]
    cs = [lax.rem(lat + d, 2) for d in range(2)]
    zs = [lax.rem(lax.div(lon, 4) + d, 4) * 4 for d in range(4)]
    xs = [lax.rem(lon + d, 4) for d in range(4)]
    return [(ys[y] + cs[c], zs[z] + xs[x]) for y, z, x, c in far_first()]


def build_left(ids_ref, valid_ref, got, taps, left, first_row, last_row):
    lat, lon = position()
    r0, c0 = offsets(ids_ref)
    low = iota((8, 128), 1) < 64


    def one_row(row):
        pr = row - 1
        u = PR * lat + pr
        holder = ((r0 + u) & 7) * N_LON
        up = pr < 0
        down = pr >= PR
        near_lat = lat + jnp.where(up, -1, jnp.where(down, 1, 0))
        near_row = jnp.where(up, PR - 1, jnp.where(down, 0, pr))
        row_ok = (near_lat >= 0) & (near_lat < N_LAT)
        near_lat = jnp.clip(near_lat, 0, N_LAT - 1)
        blocks = []
        for col in range(PC + 2):
            pc = col - 1
            b = (c0 + PC * lon + pc) & 15
            near_lon = lon + (-1 if pc < 0 else 1 if pc >= PC else 0)
            ok = row_ok & (near_lon >= 0) & (near_lon < N_LON)
            near_lon = jnp.clip(near_lon, 0, N_LON - 1)
            live = valid_ref[near_row * PC + pc % PC, near_lat * N_LON + near_lon]
            live = jnp.where(ok, live, 0)
            block = got[holder + b].astype(F32)
            blocks.append(jnp.where(live > 0, block, 0.0))
        zero = jnp.zeros((8, 128), F32)
        keep = [jnp.where(low, x, 0.0) for x in blocks]
        keep_hi = [jnp.where(low, 0.0, x) for x in blocks]
        turned = [pltpu.roll(x, 64, 1) for x in keep_hi]
        turned_hi = [pltpu.roll(x, 64, 1) for x in keep]
        for pair in range(2):
            first, second = [], []
            for q in (2 * pair, 2 * pair + 1):
                j, k = 2 * q + 1, 2 * q + 2
                main = [keep[j], keep[k], turned[j], turned[k]]
                first += main
                first += [turned_hi[j], turned_hi[k], keep_hi[j], keep_hi[k]]
                first += [zero] * 4
                first += [keep[j - 1], turned[j - 1], zero, zero]
                second += [zero] * 8
                second += main
                second += [zero, zero, keep[k + 1], turned[k + 1]]
            right = jnp.concatenate(
                [
                    jnp.concatenate(first, axis=0).astype(BF16),
                    jnp.concatenate(second, axis=0).astype(BF16),
                ],
                axis=1,
            )
            value = lax.dot_general(
                taps[...], right, (((1,), (1,)), ((), ())), preferred_element_type=F32
            ).astype(BF16)
            start = row * 64
            for side in range(2):
                for dy in range(3):
                    left[2 * pair + side, dy, pl.ds(start, 64), :] = value[
                        64 * dy : 64 * dy + 64, 128 * side : 128 * side + 128
                    ]

    for row in range(first_row, last_row):
        one_row(row)


def build_shift(bias_ref, shift):
    across = jnp.where(iota((C, C), 0) == iota((C, C), 1), bias_ref[...], 0.0)
    shift[...] = jnp.broadcast_to(jnp.sum(across, axis=1, keepdims=True), (C, 128))


def build_land(valid_ref, land):
    lat, lon = position()
    tile = lat * N_LON + lon
    lane = iota((8, 128), 1) >> 4

    def body(row, carry):
        mask = jnp.zeros((8, 128), jnp.int32)
        for pc in range(PC):
            mask = jnp.where(lane == pc, valid_ref[row * PC + pc, tile], mask)
        land[row] = mask
        return carry

    lax.fori_loop(0, PR, body, 0)


def fine_rows(first, land, left, spread, shift, stages, out, done=None):
    size = GROUP * 64
    quarter = iota((size, 128), 1) >> 5
    left_half, even_place = quarter < 2, (quarter & 1) == 0
    bias = jnp.concatenate([shift[...]] * GROUP, axis=0)
    for part, stage in enumerate(stages):
        top = first + part * GROUP
        base = pl.multiple_of((top + 1) * 64, 64)
        keep = [jnp.concatenate([land[top + r]] * 2, axis=0) > 0 for r in range(GROUP)]
        for t in range(2):
            parts = []
            for q in range(4):
                lhs = [left[q, dy, pl.ds(base, size), :] for dy in range(3)]
                if t == 0:
                    lhs.append(left[q, 0, pl.ds(base - 64, size), :])
                else:
                    lhs.append(left[q, 2, pl.ds(base + 64, size), :])
                lhs = jnp.concatenate(lhs, axis=1)
                parts.append(jnp.dot(lhs, spread[t, q], preferred_element_type=F32))
            for v in range(2):
                cut = [part[:, 128 * v : 128 * v + 128] for part in parts]
                even = [jnp.where(left_half, cut[k], cut[2 - k]) for k in (0, 2)]
                odd = [jnp.where(left_half, cut[k], cut[4 - k]) for k in (1, 3)]
                mixes = [(even[0], odd[0]), (odd[1], even[0]), (even[1], odd[1]), (odd[0], even[1])]
                for s, (first_part, second_part) in enumerate(mixes):
                    value = jnp.where(even_place, first_part, second_part)
                    if s:
                        value = pltpu.roll(value, 128 - 32 * s, 1)
                    value = value + bias
                    stage[pl.ds((8 * t + 4 * v + s) * PITCH, size), :] = value
        for r in range(GROUP):
            for o in range(C):
                block = stage[pl.ds(64 * r + o, 16, stride=PITCH), :]
                row = 16 * (part * GROUP + r)
                out[o, row : row + 16, :] = jnp.where(keep[r], block, 0.0).astype(BF16)
            if done is not None:
                done(part * GROUP + r)


def exchange_kernel(
    ids_hbm, valid_hbm, coarse_hbm, w_hbm, interp_hbm, kernel_hbm, bias_hbm,
    left, spread, early, shift, land,
    coarse, wide, rows, send, got_first, got_next, got_last, taps, stage,
    ids_ref, valid_ref, w_ref, interp_ref, kernel_ref, bias_ref, load_sem, send_sem, got_sem,
):
    lat, lon = position()
    me = lat * N_LON + lon
    sources = (
        coarse_hbm, w_hbm, ids_hbm.at[pl.ds(0, 8), :], kernel_hbm, bias_hbm, valid_hbm, interp_hbm,
    )
    places = (coarse, w_ref, ids_ref, kernel_ref, bias_ref, valid_ref, interp_ref)
    loads = [pltpu.make_async_copy(*pair, load_sem.at[k]) for k, pair in enumerate(zip(sources, places))]
    for load in loads:
        load.start()
    barrier = pltpu.get_barrier_semaphore()

    targets = peers()
    for where in targets:
        pl.semaphore_signal(barrier, inc=1, device_id=where, device_id_type=MESH)
    loads[1].wait()
    build_weights(w_ref, wide)
    for load in loads[2:]:
        load.wait()
    build_taps(kernel_ref, taps)
    build_shift(bias_ref, shift)
    build_land(valid_ref, land)
    loads[0].wait()
    pack_blocks(ids_ref, coarse, wide, rows, send)
    pl.semaphore_wait(barrier, DEVICES - 1)
    got = (got_first, got_next, got_last)
    for s in range(MOST):
        for where in targets:
            pltpu.make_async_remote_copy(
                src_ref=send.at[s, where[0] * N_LON + where[1]],
                dst_ref=got[s].at[me],
                send_sem=send_sem,
                recv_sem=got_sem.at[s],
                device_id=where,
                device_id_type=MESH,
            ).start()
        got[s][me] = send[s, me]
    build_spread(interp_ref, spread)
    others = pl.ds(0, DEVICES - 1)
    for s in range(MOST):
        pltpu.make_async_copy(send.at[s, others], got[s].at[others], got_sem.at[s]).wait()
        build_left(ids_ref, valid_ref, got[s], taps, left, 8 * s, min(8 * s + 8, PR + 2))
        if s < MOST - 1:
            rows_out = pl.ds(BATCH * 16 * s, BATCH * 16)
            stages = [stage.at[part] for part in range(PARTS)]
            fine_rows(BATCH * s, land, left, spread, shift, stages, early.at[:, rows_out, :])
    for s in range(MOST):
        pltpu.make_async_copy(send.at[s, others], got[s].at[others], send_sem).wait()


def finish_kernel(left, spread, early, shift, land, out, stage, late, early_sem, late_sem):
    head = pltpu.make_async_copy(early, out.at[:, pl.ds(0, EARLY), :], early_sem)
    head.start()
    first = 2 * BATCH

    def copy(r):
        rows_out = pl.ds(16 * (first + r), 16)
        return pltpu.make_async_copy(late.at[:, pl.ds(16 * r, 16), :], out.at[:, rows_out, :], late_sem.at[r])

    stages = [stage.at[part] for part in range(PARTS)]
    fine_rows(first, land, left, spread, shift, stages, late, lambda r: copy(r).start())
    head.wait()
    for r in range(BATCH):
        copy(r).wait()


def exchange(ids, valid, coarse, w_mix, interp, kernel, bias):
    vmem = pl.BlockSpec(memory_space=pltpu.VMEM)
    slots = (DEVICES, 8, 128)
    return pl.pallas_call(
        exchange_kernel,
        grid=(1,),
        out_shape=(
            pltpu.VMEM(LEFT, BF16),
            pltpu.VMEM((2, 4, 512, 256), BF16),
            pltpu.VMEM((C, EARLY, 128), BF16),
            pltpu.VMEM((C, 128), F32),
            pltpu.VMEM((PR, 8, 128), jnp.int32),
        ),
        in_specs=[pl.BlockSpec(memory_space=pl.ANY)] * 7,
        out_specs=(vmem,) * 5,
        scratch_shapes=[
            pltpu.VMEM((HELD, 16 * C_IN), BF16),
            pltpu.VMEM((8, 256, 128), F32),
            pltpu.VMEM((DEVICES * MOST * 8, 128), F32),
            pltpu.VMEM((MOST,) + slots, BF16),
            pltpu.VMEM(slots, BF16),
            pltpu.VMEM(slots, BF16),
            pltpu.VMEM(slots, BF16),
            pltpu.VMEM((192, 256), BF16),
            pltpu.VMEM((PARTS, 16 * PITCH, 128), F32),
            pltpu.SMEM((8, 128), jnp.int32),
            pltpu.SMEM((PR * PC, DEVICES), jnp.int32),
            pltpu.VMEM((C, C_IN), BF16),
            pltpu.VMEM((16, 256), BF16),
            pltpu.VMEM((3, 3, C, C), BF16),
            pltpu.VMEM((1, C), F32),
            pltpu.SemaphoreType.DMA((7,)),
            pltpu.SemaphoreType.DMA,
            pltpu.SemaphoreType.DMA((MOST,)),
        ],
        compiler_params=pltpu.CompilerParams(
            collective_id=0, has_side_effects=True, vmem_limit_bytes=54 * 2**20
        ),
        name="exchange",
    )(ids, valid, coarse, w_mix, interp, kernel, bias)


def finish(*arrays):
    vmem = pl.BlockSpec(memory_space=pltpu.VMEM)
    return pl.pallas_call(
        finish_kernel,
        grid=(1,),
        out_shape=jax.ShapeDtypeStruct((C, PR * 16, PC * 16), BF16),
        in_specs=[vmem] * 5,
        out_specs=pl.BlockSpec(memory_space=pl.ANY),
        scratch_shapes=[
            pltpu.VMEM((PARTS, 16 * PITCH, 128), F32),
            pltpu.VMEM((C, BATCH * 16, 128), BF16),
            pltpu.SemaphoreType.DMA,
            pltpu.SemaphoreType.DMA((BATCH,)),
        ],
        compiler_params=pltpu.CompilerParams(vmem_limit_bytes=30 * 2**20),
        name="finish",
    )(*arrays)


def per_device(coarse, w_mix, interp, kernel, bias, block_ids, valid):
    arrived = exchange(block_ids.T, valid.T, coarse, w_mix.T, interp, kernel, bias.reshape(1, C))
    return finish(*arrived)


def solution(mesh):
    placed = (P(("lat", "lon"), None), P(), P(), P(), P(), P(), P())
    return jax.shard_map(
        per_device, mesh=mesh, in_specs=placed, out_specs=P(None, "lat", "lon"), check_vma=False
    )
```

```python
import jax
import jax.numpy as jnp
from jax import lax
from jax.experimental import pallas as pl
from jax.experimental.pallas import tpu as pltpu
from jax.sharding import PartitionSpec as P

N_LAT = 8
N_LON = 16
DEVICES = N_LAT * N_LON
PR = 18
PC = 8
HELD = 960
HELD_COLS = 40
C_IN = 69
C = 64
MOST = 3
PLAN = (((0, 6),), ((6, 4), (10, 4)))
EARLY = 14 * 16
PITCH = 8 * 64 + 4
HEADS = 8
LEFT = (4, 3, (PR + 2) * 64, 128)
MESH = pl.DeviceIdType.MESH
BF16 = jnp.bfloat16
F32 = jnp.float32


def position():
    return lax.axis_index("lat"), lax.axis_index("lon")


def offsets(ids_ref):
    first = ids_ref[0, 0]
    owner = first // HELD
    local = first - owner * HELD
    row = local // HELD_COLS
    col = local - row * HELD_COLS
    return row * 8 + owner // N_LON, col * 16 + owner % N_LON


def iota(shape, dim):
    return lax.broadcasted_iota(jnp.int32, shape, dim)


def build_weights(w_ref, wide):
    wide[...] = jnp.zeros(wide.shape, F32)
    w = jnp.transpose(w_ref[...].astype(F32))
    for g in range(8):
        wide[g, 10 * g : 10 * g + C_IN, 0:C] = w
        wide[g, 10 * g + C_IN : 10 * g + 2 * C_IN, C : 2 * C] = w


def pack_blocks(ids_ref, coarse, wide, rows, send):
    a, b = position()
    r0, c0 = offsets(ids_ref)
    first_row = (a - r0) & 7
    local_row = (r0 + first_row) >> 3
    first_col = (b - c0) & 15
    local_col = (c0 + first_col) >> 4
    count = DEVICES * MOST
    slot = iota((count, 128), 0)
    tile = slot & (DEVICES - 1)
    n = ((PR * (tile >> 4) + 6 - first_row) >> 3) + (slot >> 7)
    n = jnp.clip(n, 0, PR - 1)
    m = jnp.clip((PC * (tile & 15) + PC - first_col) >> 4, 0, 7)
    col = local_col + m
    col = jnp.where(col >= HELD_COLS, col - HELD_COLS, col)
    which = (local_row + n) * HELD_COLS + col
    lane = iota((count, 128), 1)
    picks = [jnp.where(which - 128 * k == lane, 1.0, 0.0).astype(BF16) for k in range(8)]
    pick = jnp.concatenate(picks, axis=1)[:, :HELD]
    taken = jnp.dot(pick, coarse[...], preferred_element_type=F32).astype(BF16)
    for g in range(8):
        width = min(256, 16 * C_IN - 128 * g)
        part = taken[:, 128 * g : 128 * g + width]
        rows[pl.ds(g, count, stride=8), :] = jnp.dot(
            part, wide[g, :width, :].astype(BF16), preferred_element_type=F32
        )
    send[...] = rows[...].reshape(MOST, DEVICES, 8, 128).astype(BF16)


def build_spread(interp_ref, spread):
    row = iota((48, 16), 0)
    cell = 2 * (row & 7) + jnp.where(row < 32, row >> 4, (row >> 3) & 1)
    choose = jnp.where(cell == iota((48, 16), 1), 1.0, 0.0).astype(BF16)
    source = jnp.dot(choose, interp_ref[...], preferred_element_type=F32).astype(BF16)
    lane = iota((1, 256), 1)
    fine = iota((256, 256), 0)
    row_id = iota((48, 256), 0)

    def body(index, carry):
        t = index >> 2
        slot = index & 3
        fy = 8 * t + 4 * (lane >> 7) + ((lane >> 5) & 3)
        over = jnp.where(fy == 15 * t, 15 - 15 * t, -1)
        from_y = jnp.where(slot == 3, over, fy + slot - 1)
        inside = (from_y >= 0) & (from_y <= 15)
        for dx in range(3):
            from_x = (lane & 31) + (dx - 1)
            target = jnp.where(inside, from_y * 16 + (from_x & 15), -1)
            hit = jnp.where(fine == target, 1.0, 0.0).astype(BF16)
            value = jnp.dot(source, hit, preferred_element_type=F32)
            outer = (-1, 9, 2)[dx]
            patch = jnp.where(row_id < 32, (row_id >> 3) & 1, outer)
            value = jnp.where(patch == (from_x >> 4), value, 0.0)
            for q in range(4):
                for v in range(2):
                    half = value[:, 128 * v : 128 * v + 128]
                    if q:
                        half = pltpu.roll(half, 32 * q, 1)
                    half = half.astype(BF16)
                    lanes = pl.ds(128 * v, 128)
                    start = pl.multiple_of(slot * 128 + 32 * dx, 32)
                    spread[t, q, pl.ds(start, 32), lanes] = half[:32]
                    if dx != 1:
                        start = pl.multiple_of(slot * 128 + 96 + 8 * dx, 16)
                        spread[t, q, pl.ds(start, 16), lanes] = half[32:]
        return carry

    lax.fori_loop(0, 8, body, 0)


def build_taps(kernel_ref, taps):
    taps[...] = jnp.zeros(taps.shape, BF16)
    for dy in range(3):
        for dx in range(3):
            taps[64 * dy : 64 * dy + 64, 64 * dx : 64 * dx + 64] = kernel_ref[dy, dx]


def far_first():
    def hops(step):
        return sum(min(d, 4 - d) for d in step[:3])

    steps = [(y, z, x, c) for y in range(4) for z in range(4) for x in range(4) for c in range(2)]
    return sorted(steps[1:], key=hops, reverse=True)


def peers():
    lat, lon = position()
    ys = [lax.rem(lax.div(lat, 2) + d, 4) * 2 for d in range(4)]
    cs = [lax.rem(lat + d, 2) for d in range(2)]
    zs = [lax.rem(lax.div(lon, 4) + d, 4) * 4 for d in range(4)]
    xs = [lax.rem(lon + d, 4) for d in range(4)]
    return [(ys[y] + cs[c], zs[z] + xs[x]) for y, z, x, c in far_first()]


def build_left(ids_ref, valid_ref, got, taps, left, first_row, last_row):
    lat, lon = position()
    r0, c0 = offsets(ids_ref)
    low = iota((8, 128), 1) < 64


    def one_row(row):
        pr = row - 1
        u = PR * lat + pr
        holder = ((r0 + u) & 7) * N_LON
        up = pr < 0
        down = pr >= PR
        near_lat = lat + jnp.where(up, -1, jnp.where(down, 1, 0))
        near_row = jnp.where(up, PR - 1, jnp.where(down, 0, pr))
        row_ok = (near_lat >= 0) & (near_lat < N_LAT)
        near_lat = jnp.clip(near_lat, 0, N_LAT - 1)
        blocks = []
        for col in range(PC + 2):
            pc = col - 1
            b = (c0 + PC * lon + pc) & 15
            near_lon = lon + (-1 if pc < 0 else 1 if pc >= PC else 0)
            ok = row_ok & (near_lon >= 0) & (near_lon < N_LON)
            near_lon = jnp.clip(near_lon, 0, N_LON - 1)
            live = valid_ref[near_row * PC + pc % PC, near_lat * N_LON + near_lon]
            live = jnp.where(ok, live, 0)
            block = got[holder + b].astype(F32)
            blocks.append(jnp.where(live > 0, block, 0.0))
        zero = jnp.zeros((8, 128), F32)
        keep = [jnp.where(low, x, 0.0) for x in blocks]
        keep_hi = [jnp.where(low, 0.0, x) for x in blocks]
        turned = [pltpu.roll(x, 64, 1) for x in keep_hi]
        turned_hi = [pltpu.roll(x, 64, 1) for x in keep]
        for pair in range(2):
            first, second = [], []
            for q in (2 * pair, 2 * pair + 1):
                j, k = 2 * q + 1, 2 * q + 2
                main = [keep[j], keep[k], turned[j], turned[k]]
                first += main
                first += [turned_hi[j], turned_hi[k], keep_hi[j], keep_hi[k]]
                first += [zero] * 4
                first += [keep[j - 1], turned[j - 1], zero, zero]
                second += [zero] * 8
                second += main
                second += [zero, zero, keep[k + 1], turned[k + 1]]
            right = jnp.concatenate(
                [
                    jnp.concatenate(first, axis=0).astype(BF16),
                    jnp.concatenate(second, axis=0).astype(BF16),
                ],
                axis=1,
            )
            value = lax.dot_general(
                taps[...], right, (((1,), (1,)), ((), ())), preferred_element_type=F32
            ).astype(BF16)
            start = row * 64
            for side in range(2):
                for dy in range(3):
                    left[2 * pair + side, dy, pl.ds(start, 64), :] = value[
                        64 * dy : 64 * dy + 64, 128 * side : 128 * side + 128
                    ]

    for row in range(first_row, last_row):
        one_row(row)


def build_shift(bias_ref, shift):
    across = jnp.where(iota((C, C), 0) == iota((C, C), 1), bias_ref[...], 0.0)
    shift[...] = jnp.broadcast_to(jnp.sum(across, axis=1, keepdims=True), (C, 128))


def build_land(valid_ref, land):
    lat, lon = position()
    tile = lat * N_LON + lon
    lane = iota((8, 128), 1) >> 4

    def body(row, carry):
        mask = jnp.zeros((8, 128), jnp.int32)
        for pc in range(PC):
            mask = jnp.where(lane == pc, valid_ref[row * PC + pc, tile], mask)
        land[row] = mask
        return carry

    lax.fori_loop(0, PR, body, 0)


def fine_rows(first, count, land, left, spread, shift, stage, out, done=None):
    size = count * 64
    pitch = size + 4
    quarter = iota((size, 128), 1) >> 5
    left_half, even_place = quarter < 2, (quarter & 1) == 0
    bias = jnp.concatenate([shift[...]] * count, axis=0)
    base = (first + 1) * 64
    keep = [jnp.concatenate([land[first + r]] * 2, axis=0) > 0 for r in range(count)]
    for t in range(2):
        parts = []
        for q in range(4):
            lhs = [left[q, dy, pl.ds(base, size), :] for dy in range(3)]
            if t == 0:
                lhs.append(left[q, 0, pl.ds(base - 64, size), :])
            else:
                lhs.append(left[q, 2, pl.ds(base + 64, size), :])
            lhs = jnp.concatenate(lhs, axis=1)
            parts.append(jnp.dot(lhs, spread[t, q], preferred_element_type=F32))
        for v in range(2):
            cut = [part[:, 128 * v : 128 * v + 128] for part in parts]
            even = [jnp.where(left_half, cut[k], cut[2 - k]) for k in (0, 2)]
            odd = [jnp.where(left_half, cut[k], cut[4 - k]) for k in (1, 3)]
            mixes = [(even[0], odd[0]), (odd[1], even[0]), (even[1], odd[1]), (odd[0], even[1])]
            for s, (first_part, second_part) in enumerate(mixes):
                value = jnp.where(even_place, first_part, second_part)
                if s:
                    value = pltpu.roll(value, 128 - 32 * s, 1)
                value = value + bias
                stage[pl.ds((8 * t + 4 * v + s) * pitch, size), :] = value
    for r in range(count):
        for o in range(C):
            block = stage[pl.ds(64 * r + o, 16, stride=pitch), :]
            row = 16 * r
            out[o, row : row + 16, :] = jnp.where(keep[r], block, 0.0).astype(BF16)
        if done is not None:
            done(r)


def exchange_kernel(
    ids_hbm, valid_hbm, coarse_hbm, w_hbm, interp_hbm, kernel_hbm, bias_hbm,
    left, spread, early, shift, land,
    coarse, wide, rows, send, got_first, got_next, got_last, taps, stage,
    ids_ref, valid_ref, w_ref, interp_ref, kernel_ref, bias_ref, load_sem, send_sem, got_sem,
):
    lat, lon = position()
    me = lat * N_LON + lon
    sources = (
        coarse_hbm, w_hbm, ids_hbm.at[pl.ds(0, 8), :], kernel_hbm, bias_hbm, valid_hbm, interp_hbm,
    )
    places = (coarse, w_ref, ids_ref, kernel_ref, bias_ref, valid_ref, interp_ref)
    loads = [pltpu.make_async_copy(*pair, load_sem.at[k]) for k, pair in enumerate(zip(sources, places))]
    for load in loads:
        load.start()
    barrier = pltpu.get_barrier_semaphore()

    targets = peers()
    for where in targets:
        pl.semaphore_signal(barrier, inc=1, device_id=where, device_id_type=MESH)
    loads[1].wait()
    build_weights(w_ref, wide)
    for load in loads[2:]:
        load.wait()
    build_taps(kernel_ref, taps)
    build_shift(bias_ref, shift)
    build_land(valid_ref, land)
    loads[0].wait()
    pack_blocks(ids_ref, coarse, wide, rows, send)
    pl.semaphore_wait(barrier, DEVICES - 1)
    got = (got_first, got_next, got_last)
    for s in range(MOST):
        for where in targets:
            pltpu.make_async_remote_copy(
                src_ref=send.at[s, where[0] * N_LON + where[1]],
                dst_ref=got[s].at[me],
                send_sem=send_sem,
                recv_sem=got_sem.at[s],
                device_id=where,
                device_id_type=MESH,
            ).start()
        got[s][me] = send[s, me]
    build_spread(interp_ref, spread)
    others = pl.ds(0, DEVICES - 1)
    for s in range(MOST):
        pltpu.make_async_copy(send.at[s, others], got[s].at[others], got_sem.at[s]).wait()
        build_left(ids_ref, valid_ref, got[s], taps, left, 8 * s, min(8 * s + 8, PR + 2))
        if s < MOST - 1:
            for first, count in PLAN[s]:
                rows_out = pl.ds(16 * first, 16 * count)
                fine_rows(first, count, land, left, spread, shift, stage, early.at[:, rows_out, :])
    for s in range(MOST):
        pltpu.make_async_copy(send.at[s, others], got[s].at[others], send_sem).wait()


def finish_kernel(left, spread, early, shift, land, out, stage, late, early_sem, late_sem):
    heads = []
    for k in range(HEADS):
        part = pl.ds(C // HEADS * k, C // HEADS)
        there = out.at[part, pl.ds(0, EARLY), :]
        heads.append(pltpu.make_async_copy(early.at[part], there, early_sem.at[k]))
        heads[-1].start()
    first = EARLY // 16
    count = PR - first

    def copy(r):
        rows_out = pl.ds(16 * (first + r), 16)
        return pltpu.make_async_copy(late.at[:, pl.ds(16 * r, 16), :], out.at[:, rows_out, :], late_sem.at[r])

    fine_rows(first, count, land, left, spread, shift, stage, late, lambda r: copy(r).start())
    for head in heads:
        head.wait()
    for r in range(count):
        copy(r).wait()


def exchange(ids, valid, coarse, w_mix, interp, kernel, bias):
    vmem = pl.BlockSpec(memory_space=pltpu.VMEM)
    slots = (DEVICES, 8, 128)
    return pl.pallas_call(
        exchange_kernel,
        grid=(1,),
        out_shape=(
            pltpu.VMEM(LEFT, BF16),
            pltpu.VMEM((2, 4, 512, 256), BF16),
            pltpu.VMEM((C, EARLY, 128), BF16),
            pltpu.VMEM((C, 128), F32),
            pltpu.VMEM((PR, 8, 128), jnp.int32),
        ),
        in_specs=[pl.BlockSpec(memory_space=pl.ANY)] * 7,
        out_specs=(vmem,) * 5,
        scratch_shapes=[
            pltpu.VMEM((HELD, 16 * C_IN), BF16),
            pltpu.VMEM((8, 256, 128), F32),
            pltpu.VMEM((DEVICES * MOST * 8, 128), F32),
            pltpu.VMEM((MOST,) + slots, BF16),
            pltpu.VMEM(slots, BF16),
            pltpu.VMEM(slots, BF16),
            pltpu.VMEM(slots, BF16),
            pltpu.VMEM((192, 256), BF16),
            pltpu.VMEM((16 * PITCH, 128), F32),
            pltpu.SMEM((8, 128), jnp.int32),
            pltpu.SMEM((PR * PC, DEVICES), jnp.int32),
            pltpu.VMEM((C, C_IN), BF16),
            pltpu.VMEM((16, 256), BF16),
            pltpu.VMEM((3, 3, C, C), BF16),
            pltpu.VMEM((1, C), F32),
            pltpu.SemaphoreType.DMA((7,)),
            pltpu.SemaphoreType.DMA,
            pltpu.SemaphoreType.DMA((MOST,)),
        ],
        compiler_params=pltpu.CompilerParams(
            collective_id=0, has_side_effects=True, vmem_limit_bytes=53 * 2**20
        ),
        name="exchange",
    )(ids, valid, coarse, w_mix, interp, kernel, bias)


def finish(*arrays):
    vmem = pl.BlockSpec(memory_space=pltpu.VMEM)
    return pl.pallas_call(
        finish_kernel,
        grid=(1,),
        out_shape=jax.ShapeDtypeStruct((C, PR * 16, PC * 16), BF16),
        in_specs=[vmem] * 5,
        out_specs=pl.BlockSpec(memory_space=pl.ANY),
        scratch_shapes=[
            pltpu.VMEM((16 * PITCH, 128), F32),
            pltpu.VMEM((C, PR * 16 - EARLY, 128), BF16),
            pltpu.SemaphoreType.DMA((HEADS,)),
            pltpu.SemaphoreType.DMA((PR - EARLY // 16,)),
        ],
        compiler_params=pltpu.CompilerParams(vmem_limit_bytes=30 * 2**20),
        name="finish",
    )(*arrays)


def per_device(coarse, w_mix, interp, kernel, bias, block_ids, valid):
    arrived = exchange(block_ids.T, valid.T, coarse, w_mix.T, interp, kernel, bias.reshape(1, C))
    return finish(*arrived)


def solution(mesh):
    placed = (P(("lat", "lon"), None), P(), P(), P(), P(), P(), P())
    return jax.shard_map(
        per_device, mesh=mesh, in_specs=placed, out_specs=P(None, "lat", "lon"), check_vma=False
    )
```

```python
import jax
import jax.numpy as jnp
from jax import lax
from jax.experimental import pallas as pl
from jax.experimental.pallas import tpu as pltpu
from jax.sharding import PartitionSpec as P

N_LAT = 8
N_LON = 16
DEVICES = N_LAT * N_LON
PR = 18
PC = 8
HELD = 960
HELD_COLS = 40
C_IN = 69
C = 64
MOST = 3
PLAN = (((0, 6),), ((6, 4), (10, 4)))
EARLY = 14 * 16
PITCH = 8 * 64 + 4
HEADS = 4
LEFT = (4, 3, (PR + 2) * 64, 128)
MESH = pl.DeviceIdType.MESH
BF16 = jnp.bfloat16
F32 = jnp.float32


def position():
    return lax.axis_index("lat"), lax.axis_index("lon")


def offsets(ids_ref):
    first = ids_ref[0, 0]
    owner = first // HELD
    local = first - owner * HELD
    row = local // HELD_COLS
    col = local - row * HELD_COLS
    return row * 8 + owner // N_LON, col * 16 + owner % N_LON


def iota(shape, dim):
    return lax.broadcasted_iota(jnp.int32, shape, dim)


def build_weights(w_ref, wide):
    wide[...] = jnp.zeros(wide.shape, F32)
    w = jnp.transpose(w_ref[...].astype(F32))
    for g in range(8):
        wide[g, 10 * g : 10 * g + C_IN, 0:C] = w
        wide[g, 10 * g + C_IN : 10 * g + 2 * C_IN, C : 2 * C] = w


def pack_blocks(ids_ref, coarse, wide, rows, send):
    a, b = position()
    r0, c0 = offsets(ids_ref)
    first_row = (a - r0) & 7
    local_row = (r0 + first_row) >> 3
    first_col = (b - c0) & 15
    local_col = (c0 + first_col) >> 4
    count = DEVICES * MOST
    slot = iota((count, 128), 0)
    tile = slot & (DEVICES - 1)
    n = ((PR * (tile >> 4) + 6 - first_row) >> 3) + (slot >> 7)
    n = jnp.clip(n, 0, PR - 1)
    m = jnp.clip((PC * (tile & 15) + PC - first_col) >> 4, 0, 7)
    col = local_col + m
    col = jnp.where(col >= HELD_COLS, col - HELD_COLS, col)
    which = (local_row + n) * HELD_COLS + col
    lane = iota((count, 128), 1)
    picks = [jnp.where(which - 128 * k == lane, 1.0, 0.0).astype(BF16) for k in range(8)]
    pick = jnp.concatenate(picks, axis=1)[:, :HELD]
    taken = jnp.dot(pick, coarse[...], preferred_element_type=F32).astype(BF16)
    for g in range(8):
        width = min(256, 16 * C_IN - 128 * g)
        part = taken[:, 128 * g : 128 * g + width]
        rows[pl.ds(g, count, stride=8), :] = jnp.dot(
            part, wide[g, :width, :].astype(BF16), preferred_element_type=F32
        )
    send[...] = rows[...].reshape(MOST, DEVICES, 8, 128).astype(BF16)


def build_spread(interp_ref, spread):
    row = iota((48, 16), 0)
    cell = 2 * (row & 7) + jnp.where(row < 32, row >> 4, (row >> 3) & 1)
    choose = jnp.where(cell == iota((48, 16), 1), 1.0, 0.0).astype(BF16)
    source = jnp.dot(choose, interp_ref[...], preferred_element_type=F32).astype(BF16)
    lane = iota((1, 256), 1)
    fine = iota((256, 256), 0)
    row_id = iota((48, 256), 0)

    def body(index, carry):
        t = index >> 2
        slot = index & 3
        fy = 8 * t + 4 * (lane >> 7) + ((lane >> 5) & 3)
        over = jnp.where(fy == 15 * t, 15 - 15 * t, -1)
        from_y = jnp.where(slot == 3, over, fy + slot - 1)
        inside = (from_y >= 0) & (from_y <= 15)
        for dx in range(3):
            from_x = (lane & 31) + (dx - 1)
            target = jnp.where(inside, from_y * 16 + (from_x & 15), -1)
            hit = jnp.where(fine == target, 1.0, 0.0).astype(BF16)
            value = jnp.dot(source, hit, preferred_element_type=F32)
            outer = (-1, 9, 2)[dx]
            patch = jnp.where(row_id < 32, (row_id >> 3) & 1, outer)
            value = jnp.where(patch == (from_x >> 4), value, 0.0)
            for q in range(4):
                for v in range(2):
                    half = value[:, 128 * v : 128 * v + 128]
                    if q:
                        half = pltpu.roll(half, 32 * q, 1)
                    half = half.astype(BF16)
                    lanes = pl.ds(128 * v, 128)
                    start = pl.multiple_of(slot * 128 + 32 * dx, 32)
                    spread[t, q, pl.ds(start, 32), lanes] = half[:32]
                    if dx != 1:
                        start = pl.multiple_of(slot * 128 + 96 + 8 * dx, 16)
                        spread[t, q, pl.ds(start, 16), lanes] = half[32:]
        return carry

    lax.fori_loop(0, 8, body, 0)


def build_taps(kernel_ref, taps):
    taps[...] = jnp.zeros(taps.shape, BF16)
    for dy in range(3):
        for dx in range(3):
            taps[64 * dy : 64 * dy + 64, 64 * dx : 64 * dx + 64] = kernel_ref[dy, dx]


def far_first():
    def hops(step):
        return sum(min(d, 4 - d) for d in step[:3])

    steps = [(y, z, x, c) for y in range(4) for z in range(4) for x in range(4) for c in range(2)]
    return sorted(steps[1:], key=hops, reverse=True)


def peers():
    lat, lon = position()
    ys = [lax.rem(lax.div(lat, 2) + d, 4) * 2 for d in range(4)]
    cs = [lax.rem(lat + d, 2) for d in range(2)]
    zs = [lax.rem(lax.div(lon, 4) + d, 4) * 4 for d in range(4)]
    xs = [lax.rem(lon + d, 4) for d in range(4)]
    return [(ys[y] + cs[c], zs[z] + xs[x]) for y, z, x, c in far_first()]


def build_left(ids_ref, valid_ref, got, taps, left, first_row, last_row):
    lat, lon = position()
    r0, c0 = offsets(ids_ref)
    low = iota((8, 128), 1) < 64


    def one_row(row):
        pr = row - 1
        u = PR * lat + pr
        holder = ((r0 + u) & 7) * N_LON
        up = pr < 0
        down = pr >= PR
        near_lat = lat + jnp.where(up, -1, jnp.where(down, 1, 0))
        near_row = jnp.where(up, PR - 1, jnp.where(down, 0, pr))
        row_ok = (near_lat >= 0) & (near_lat < N_LAT)
        near_lat = jnp.clip(near_lat, 0, N_LAT - 1)
        blocks = []
        for col in range(PC + 2):
            pc = col - 1
            b = (c0 + PC * lon + pc) & 15
            near_lon = lon + (-1 if pc < 0 else 1 if pc >= PC else 0)
            ok = row_ok & (near_lon >= 0) & (near_lon < N_LON)
            near_lon = jnp.clip(near_lon, 0, N_LON - 1)
            live = valid_ref[near_row * PC + pc % PC, near_lat * N_LON + near_lon]
            live = jnp.where(ok, live, 0)
            block = got[holder + b].astype(F32)
            blocks.append(jnp.where(live > 0, block, 0.0))
        zero = jnp.zeros((8, 128), F32)
        keep = [jnp.where(low, x, 0.0) for x in blocks]
        keep_hi = [jnp.where(low, 0.0, x) for x in blocks]
        turned = [pltpu.roll(x, 64, 1) for x in keep_hi]
        turned_hi = [pltpu.roll(x, 64, 1) for x in keep]
        for pair in range(2):
            first, second = [], []
            for q in (2 * pair, 2 * pair + 1):
                j, k = 2 * q + 1, 2 * q + 2
                main = [keep[j], keep[k], turned[j], turned[k]]
                first += main
                first += [turned_hi[j], turned_hi[k], keep_hi[j], keep_hi[k]]
                first += [zero] * 4
                first += [keep[j - 1], turned[j - 1], zero, zero]
                second += [zero] * 8
                second += main
                second += [zero, zero, keep[k + 1], turned[k + 1]]
            right = jnp.concatenate(
                [
                    jnp.concatenate(first, axis=0).astype(BF16),
                    jnp.concatenate(second, axis=0).astype(BF16),
                ],
                axis=1,
            )
            value = lax.dot_general(
                taps[...], right, (((1,), (1,)), ((), ())), preferred_element_type=F32
            ).astype(BF16)
            start = row * 64
            for side in range(2):
                for dy in range(3):
                    left[2 * pair + side, dy, pl.ds(start, 64), :] = value[
                        64 * dy : 64 * dy + 64, 128 * side : 128 * side + 128
                    ]

    for row in range(first_row, last_row):
        one_row(row)


def build_shift(bias_ref, shift):
    across = jnp.where(iota((C, C), 0) == iota((C, C), 1), bias_ref[...], 0.0)
    shift[...] = jnp.broadcast_to(jnp.sum(across, axis=1, keepdims=True), (C, 128))


def build_land(valid_ref, land):
    lat, lon = position()
    tile = lat * N_LON + lon
    lane = iota((8, 128), 1) >> 4

    def body(row, carry):
        mask = jnp.zeros((8, 128), jnp.int32)
        for pc in range(PC):
            mask = jnp.where(lane == pc, valid_ref[row * PC + pc, tile], mask)
        land[row] = mask
        return carry

    lax.fori_loop(0, PR, body, 0)


def fine_rows(first, count, land, left, spread, shift, stage, out, done=None):
    size = count * 64
    pitch = size + 4
    quarter = iota((size, 128), 1) >> 5
    left_half, even_place = quarter < 2, (quarter & 1) == 0
    bias = jnp.concatenate([shift[...]] * count, axis=0)
    base = (first + 1) * 64
    keep = [jnp.concatenate([land[first + r]] * 2, axis=0) > 0 for r in range(count)]
    for t in range(2):
        parts = []
        for q in range(4):
            lhs = [left[q, dy, pl.ds(base, size), :] for dy in range(3)]
            if t == 0:
                lhs.append(left[q, 0, pl.ds(base - 64, size), :])
            else:
                lhs.append(left[q, 2, pl.ds(base + 64, size), :])
            lhs = jnp.concatenate(lhs, axis=1)
            parts.append(jnp.dot(lhs, spread[t, q], preferred_element_type=F32))
        for v in range(2):
            cut = [part[:, 128 * v : 128 * v + 128] for part in parts]
            even = [jnp.where(left_half, cut[k], cut[2 - k]) for k in (0, 2)]
            odd = [jnp.where(left_half, cut[k], cut[4 - k]) for k in (1, 3)]
            mixes = [(even[0], odd[0]), (odd[1], even[0]), (even[1], odd[1]), (odd[0], even[1])]
            for s, (first_part, second_part) in enumerate(mixes):
                value = jnp.where(even_place, first_part, second_part)
                if s:
                    value = pltpu.roll(value, 128 - 32 * s, 1)
                value = value + bias
                stage[pl.ds((8 * t + 4 * v + s) * pitch, size), :] = value
    for r in range(count):
        for o in range(C):
            block = stage[pl.ds(64 * r + o, 16, stride=pitch), :]
            row = 16 * r
            out[o, row : row + 16, :] = jnp.where(keep[r], block, 0.0).astype(BF16)
        if done is not None:
            done(r)


def exchange_kernel(
    ids_hbm, valid_hbm, coarse_hbm, w_hbm, interp_hbm, kernel_hbm, bias_hbm,
    left, spread, early, shift, land,
    coarse, wide, rows, send, got_first, got_next, got_last, taps, stage,
    ids_ref, valid_ref, w_ref, interp_ref, kernel_ref, bias_ref, load_sem, send_sem, got_sem,
):
    lat, lon = position()
    me = lat * N_LON + lon
    sources = (
        coarse_hbm, w_hbm, ids_hbm.at[pl.ds(0, 8), :], kernel_hbm, bias_hbm, valid_hbm, interp_hbm,
    )
    places = (coarse, w_ref, ids_ref, kernel_ref, bias_ref, valid_ref, interp_ref)
    loads = [pltpu.make_async_copy(*pair, load_sem.at[k]) for k, pair in enumerate(zip(sources, places))]
    for load in loads:
        load.start()
    barrier = pltpu.get_barrier_semaphore()

    targets = peers()
    for where in targets:
        pl.semaphore_signal(barrier, inc=1, device_id=where, device_id_type=MESH)
    loads[1].wait()
    build_weights(w_ref, wide)
    for load in loads[2:]:
        load.wait()
    build_taps(kernel_ref, taps)
    build_shift(bias_ref, shift)
    build_land(valid_ref, land)
    loads[0].wait()
    pack_blocks(ids_ref, coarse, wide, rows, send)
    pl.semaphore_wait(barrier, DEVICES - 1)
    got = (got_first, got_next, got_last)
    for s in range(MOST):
        for where in targets:
            pltpu.make_async_remote_copy(
                src_ref=send.at[s, where[0] * N_LON + where[1]],
                dst_ref=got[s].at[me],
                send_sem=send_sem,
                recv_sem=got_sem.at[s],
                device_id=where,
                device_id_type=MESH,
            ).start()
        got[s][me] = send[s, me]
    build_spread(interp_ref, spread)
    others = pl.ds(0, DEVICES - 1)
    for s in range(MOST):
        pltpu.make_async_copy(send.at[s, others], got[s].at[others], got_sem.at[s]).wait()
        build_left(ids_ref, valid_ref, got[s], taps, left, 8 * s, min(8 * s + 8, PR + 2))
        if s < MOST - 1:
            for first, count in PLAN[s]:
                rows_out = pl.ds(16 * first, 16 * count)
                fine_rows(first, count, land, left, spread, shift, stage, early.at[:, rows_out, :])
    for s in range(MOST):
        pltpu.make_async_copy(send.at[s, others], got[s].at[others], send_sem).wait()


def finish_kernel(left, spread, early, shift, land, out, stage, late, early_sem, late_sem):
    heads = []
    for k in range(HEADS):
        part = pl.ds(C // HEADS * k, C // HEADS)
        there = out.at[part, pl.ds(0, EARLY), :]
        heads.append(pltpu.make_async_copy(early.at[part], there, early_sem.at[k]))
        heads[-1].start()
    first = EARLY // 16
    count = PR - first

    def copy(r):
        rows_out = pl.ds(16 * (first + r), 16)
        return pltpu.make_async_copy(late.at[:, pl.ds(16 * r, 16), :], out.at[:, rows_out, :], late_sem.at[r])

    fine_rows(first, count, land, left, spread, shift, stage, late, lambda r: copy(r).start())
    for head in heads:
        head.wait()
    for r in range(count):
        copy(r).wait()


def exchange(ids, valid, coarse, w_mix, interp, kernel, bias):
    vmem = pl.BlockSpec(memory_space=pltpu.VMEM)
    slots = (DEVICES, 8, 128)
    return pl.pallas_call(
        exchange_kernel,
        grid=(1,),
        out_shape=(
            pltpu.VMEM(LEFT, BF16),
            pltpu.VMEM((2, 4, 512, 256), BF16),
            pltpu.VMEM((C, EARLY, 128), BF16),
            pltpu.VMEM((C, 128), F32),
            pltpu.VMEM((PR, 8, 128), jnp.int32),
        ),
        in_specs=[pl.BlockSpec(memory_space=pl.ANY)] * 7,
        out_specs=(vmem,) * 5,
        scratch_shapes=[
            pltpu.VMEM((HELD, 16 * C_IN), BF16),
            pltpu.VMEM((8, 256, 128), F32),
            pltpu.VMEM((DEVICES * MOST * 8, 128), F32),
            pltpu.VMEM((MOST,) + slots, BF16),
            pltpu.VMEM(slots, BF16),
            pltpu.VMEM(slots, BF16),
            pltpu.VMEM(slots, BF16),
            pltpu.VMEM((192, 256), BF16),
            pltpu.VMEM((16 * PITCH, 128), F32),
            pltpu.SMEM((8, 128), jnp.int32),
            pltpu.SMEM((PR * PC, DEVICES), jnp.int32),
            pltpu.VMEM((C, C_IN), BF16),
            pltpu.VMEM((16, 256), BF16),
            pltpu.VMEM((3, 3, C, C), BF16),
            pltpu.VMEM((1, C), F32),
            pltpu.SemaphoreType.DMA((7,)),
            pltpu.SemaphoreType.DMA,
            pltpu.SemaphoreType.DMA((MOST,)),
        ],
        compiler_params=pltpu.CompilerParams(
            collective_id=0, has_side_effects=True, vmem_limit_bytes=53 * 2**20
        ),
        name="exchange",
    )(ids, valid, coarse, w_mix, interp, kernel, bias)


def finish(*arrays):
    vmem = pl.BlockSpec(memory_space=pltpu.VMEM)
    return pl.pallas_call(
        finish_kernel,
        grid=(1,),
        out_shape=jax.ShapeDtypeStruct((C, PR * 16, PC * 16), BF16),
        in_specs=[vmem] * 5,
        out_specs=pl.BlockSpec(memory_space=pl.ANY),
        scratch_shapes=[
            pltpu.VMEM((16 * PITCH, 128), F32),
            pltpu.VMEM((C, PR * 16 - EARLY, 128), BF16),
            pltpu.SemaphoreType.DMA((HEADS,)),
            pltpu.SemaphoreType.DMA((PR - EARLY // 16,)),
        ],
        compiler_params=pltpu.CompilerParams(vmem_limit_bytes=30 * 2**20),
        name="finish",
    )(*arrays)


def per_device(coarse, w_mix, interp, kernel, bias, block_ids, valid):
    arrived = exchange(block_ids.T, valid.T, coarse, w_mix.T, interp, kernel, bias.reshape(1, C))
    return finish(*arrived)


def solution(mesh):
    placed = (P(("lat", "lon"), None), P(), P(), P(), P(), P(), P())
    return jax.shard_map(
        per_device, mesh=mesh, in_specs=placed, out_specs=P(None, "lat", "lon"), check_vma=False
    )
```
